128 devices in a mesh: rows: 32 (over y, x, core), cols: 4 (over z).
Axes of the slice: x: 4, y: 4, z: 4, core: 2. Of those that a mesh axis runs over, the one named last changes fastest.
Arguments:
- token_ids: int32 [64, 2048], P('rows', 'cols'), may hold values from 0 to 524287, as said below
- lengths: int32 [64], P('rows'), may hold values from 1 to 2048
- table: bfloat16 [524288, 512], P('rows', 'cols'), may hold values from -6 to 6
- attn_gain: float32 [512], replicated, may hold values from 0.1 to 1.9
- w_qkv: bfloat16 [512, 1536], replicated, may hold values from -2 to 2
- w_out: bfloat16 [512, 512], replicated, may hold values from -0.25 to 0.25
- mlp_gain: float32 [512], replicated, may hold values from 0.1 to 1.9
- w_in: bfloat16 [512, 4096], replicated, may hold values from -0.25 to 0.25
- w_down: bfloat16 [2048, 512], replicated, may hold values from -0.125 to 0.125
Outputs:
- layer_out: bfloat16 [64, 2048, 512], P('rows', 'cols')
The draws below stay inside these ranges and needn't reach their ends.
Inputs may be any that keep to these rules, and one draw needn't show every extreme that they name: `token_ids`: ids lie in 0 to 524287. In each aligned block of 2 histories (4096 positions) at most 341 ids fall in any one block of 16384 consecutive table rows, and in every such block of histories some block of table rows receives exactly 341.
All inputs are finite; a program needn't handle non-finite values.
Results may differ from the reference program's by a relative error of at most 0.012.
Values may be sent and summed in bfloat16 or wider, within the bound.
No kernel may reach another device: no remote copies, remote signals or barrier semaphores. Data moves between devices by JAX's collectives and lax.ppermute only.
A program may use at most 192 MiB of HBM per device.

```python
import jax
import jax.numpy as jnp
from jax import lax

D = 512
HEADS = 8
FF = 2048
VOC_DEV = 16384
BD = 2
L = 2048
B = 64
VOCAB = 524288
CAP = 341


def one_block(key):
    key_hot, key_order, key_shuffle, key_offset = jax.random.split(key, 4)
    block_count = B // BD
    token_count = BD * L
    hot_block = jax.random.randint(key_hot, (), 0, block_count)
    slot_ids = jnp.arange(block_count * CAP, dtype=jnp.int32)
    slot_block = slot_ids // CAP
    order_rank = jax.random.permutation(key_order, block_count * CAP).astype(jnp.int32)
    priority = jnp.where(slot_block == hot_block, 0, 1) * (block_count * CAP) + order_rank
    chosen_order = jnp.argsort(priority)
    chosen_block = slot_block[chosen_order[:token_count]]
    chosen_block = jax.random.permutation(key_shuffle, chosen_block)
    offsets = jax.random.randint(key_offset, (token_count,), 0, VOC_DEV)
    return (chosen_block * VOC_DEV + offsets).astype(jnp.int32).reshape(BD, L)


def draw_token_ids(key, part):
    keys = jax.random.split(jax.random.fold_in(key, 11), B // BD)
    return jax.vmap(one_block)(keys).reshape(B, L)


def draw_w_qkv(key, part):
    key_base = jax.random.fold_in(jax.random.fold_in(key, 23), 0)
    base = jnp.clip(jax.random.normal(key_base, (D, 3 * D), jnp.float32), -5.0, 5.0) / jnp.sqrt(1.0 * D)
    return jnp.clip(base, -2.0, 2.0).astype(jnp.bfloat16)


def touch_ends(drawn, stream_key, low, top_value):
    longest = drawn.shape.index(max(drawn.shape))
    spots = []
    for shift in (0, 1):
        where = [jax.random.randint(jax.random.fold_in(stream_key, axis), (), 0, length) for axis, length in enumerate(drawn.shape)]
        where[longest] = (where[longest] + shift) % drawn.shape[longest]
        spots.append(tuple(where))
    return drawn.at[spots[0]].set(low).at[spots[1]].set(top_value)


def block_scale(stream_key, extent, shards, low, largest):
    loudness = 1.0
    for axis_at, parts in shards:
        draws = jax.random.uniform(jax.random.fold_in(jax.random.fold_in(stream_key, 6), axis_at), (parts,), jnp.float32, low / len(shards), largest / len(shards))
        loudness = loudness * jnp.repeat(jnp.exp(draws), extent[axis_at] // parts).reshape((-1,) + (1,) * (len(extent) - 1 - axis_at))
    return loudness


def centred(key, shape, scale, most, cuts=(), kind=jnp.bfloat16):
    factor_of = block_scale(key, shape, cuts, -0.22, 0.18) if cuts else 1.0
    entries = jax.random.normal(key, shape, jnp.float32) * scale * factor_of
    return jnp.minimum(jnp.maximum(entries, -most), most).astype(kind)


def setup_inputs(seed: int = 0) -> dict:
    streams_of = jax.random.split(jax.random.key(seed), 10)
    return {
        "token_ids": draw_token_ids(jax.random.fold_in(streams_of[9], 71), 0),
        "lengths": touch_ends(jax.random.randint(streams_of[1], (B,), 1, L + 1), jax.random.fold_in(streams_of[1], 1), 1, L).astype(jnp.int32),
        "table": centred(streams_of[2], (VOCAB, D), 1.0, 6.0, ((0, 32), (1, 4))),
        "attn_gain": jnp.clip(1.0 + 0.18 * jax.random.normal(streams_of[3], (D,), jnp.float32), 0.1, 1.9),
        "w_qkv": draw_w_qkv(jax.random.fold_in(streams_of[9], 71), 0),
        "w_out": centred(streams_of[5], (D, D), D ** -0.5, 0.25),
        "mlp_gain": jnp.clip(1.0 + 0.18 * jax.random.normal(streams_of[6], (D,), jnp.float32), 0.1, 1.9),
        "w_in": centred(streams_of[7], (D, 2 * FF), D ** -0.5, 0.25),
        "w_down": centred(streams_of[8], (FF, D), FF ** -0.5, 0.125),
    }


def rms_norm(values_f32, gain):
    mean_sq = lax.optimization_barrier(jnp.mean(values_f32 * values_f32, axis=-1, keepdims=True))
    return values_f32 * lax.rsqrt(mean_sq + 1e-06) * gain

def layer(sequence, length, attn_gain, w_qkv, w_out, mlp_gain, w_in, w_down):
    residual = sequence.astype(jnp.float32)
    normed = rms_norm(residual, attn_gain).astype(jnp.bfloat16)
    projected = jnp.dot(normed, w_qkv, preferred_element_type=jnp.float32).astype(jnp.bfloat16)
    head_dim = D // HEADS
    queries = projected[:, :D].reshape(L, HEADS, head_dim).astype(jnp.float32)
    keys = projected[:, D:2 * D].reshape(L, HEADS, head_dim).astype(jnp.float32)
    values = projected[:, 2 * D:].reshape(L, HEADS, head_dim).astype(jnp.float32)
    scores = jnp.einsum('qhd,khd->hqk', queries, keys) * 0.125
    position = jnp.arange(L, dtype=jnp.int32)
    valid = (position[None, :] <= position[:, None]) & (position[None, :] < length)
    valid = valid[None, :, :]
    scores = jnp.where(valid, scores, -1e+30)
    row_max = lax.optimization_barrier(jnp.max(scores, axis=-1, keepdims=True))
    probs = jnp.where(valid, jnp.exp(scores - row_max), 0.0)
    total = lax.optimization_barrier(jnp.sum(probs, axis=-1))
    weights = probs.astype(jnp.bfloat16).astype(jnp.float32)
    summed = jnp.einsum('hqk,khd->hqd', weights, values) / total[..., None]
    attended = jnp.transpose(summed, (1, 0, 2)).reshape(L, D).astype(jnp.bfloat16)
    hidden = (residual + jnp.dot(attended, w_out, preferred_element_type=jnp.float32)).astype(jnp.bfloat16)
    hidden_f32 = hidden.astype(jnp.float32)
    normed_two = rms_norm(hidden_f32, mlp_gain).astype(jnp.bfloat16)
    gate_up = jnp.dot(normed_two, w_in, preferred_element_type=jnp.float32)
    act = (jax.nn.silu(gate_up[:, :FF]) * gate_up[:, FF:]).astype(jnp.bfloat16)
    return (hidden_f32 + jnp.dot(act, w_down, preferred_element_type=jnp.float32)).astype(jnp.bfloat16)

def reference(token_ids, lengths, table, attn_gain, w_qkv, w_out, mlp_gain, w_in, w_down):
    embedded = jnp.take(table, token_ids, axis=0)

    def one_history(pair):
        sequence, length = pair
        return layer(sequence, length, attn_gain, w_qkv, w_out, mlp_gain, w_in, w_down)
    return lax.map(one_history, (embedded, lengths))
```

```python
import functools

import jax
import jax.numpy as jnp
from jax import lax
from jax.experimental import pallas as pl
from jax.experimental.pallas import tpu as pltpu
from jax.sharding import PartitionSpec as P

D = 512
HEADS = 8
FF = 2048
CAP = 344
REQ = 384
LOG2E = 1.4426950408889634
SWAP = [(0, 1), (1, 0), (2, 3), (3, 2)]
CROSS = [(0, 3), (3, 0), (1, 2), (2, 1)]
VM = pl.BlockSpec(memory_space=pltpu.VMEM)
SM = pl.BlockSpec(memory_space=pltpu.SMEM)
F32 = jnp.float32
BF = jnp.bfloat16
I32 = jnp.int32


def dot(a, b):
    return lax.dot_general(a, b, (((1,), (0,)), ((), ())), preferred_element_type=F32)


def dot_t(a, b):
    return lax.dot_general(a, b, (((1,), (1,)), ((), ())), preferred_element_type=F32)


def params(mib):
    return pltpu.CompilerParams(vmem_limit_bytes=mib * 1024 * 1024)


def route_kernel(row_bits, owners, ids_ref, slot_ref, req_ref):
    rows, width = ids_ref.shape
    parts = REQ // 128
    upper = (
        lax.broadcasted_iota(I32, (width, width), 0) < lax.broadcasted_iota(I32, (width, width), 1)
    ).astype(BF)
    owner_iota = lax.broadcasted_iota(I32, (owners, width), 0)
    group_iota = lax.broadcasted_iota(I32, (owners * parts, width), 0)
    lane_iota = lax.broadcasted_iota(I32, (128, width), 0)
    carry = jnp.zeros((owners, 1), F32)
    total = jnp.zeros((owners * parts, 256), F32)
    for r in range(rows):
        ids = ids_ref[r : r + 1, :]
        owner = lax.shift_right_logical(ids, row_bits)
        offset = ids & ((1 << row_bits) - 1)
        hot = (owner_iota == owner).astype(F32)
        before = dot(hot.astype(BF), upper) + carry
        rank = jnp.sum(hot * before, axis=0, keepdims=True).astype(I32)
        carry = carry + jnp.sum(hot, axis=1, keepdims=True)
        slot_ref[r : r + 1, :] = owner * CAP + rank
        group = owner * parts + lax.shift_right_logical(rank, 7)
        in_group = (group_iota == group).astype(BF)
        at_lane = lane_iota == (rank & 127)
        high = jnp.where(at_lane, lax.shift_right_logical(offset, 7), 0).astype(F32).astype(BF)
        low = jnp.where(at_lane, offset & 127, 0).astype(F32).astype(BF)
        total = total + dot_t(in_group, jnp.concatenate([high, low], axis=0))
    count = carry.astype(I32)
    last_group = (
        lax.broadcasted_iota(I32, (owners * parts, owners), 0)
        == lax.broadcasted_iota(I32, (owners * parts, owners), 1) * parts + parts - 1
    ).astype(BF)
    lane = lax.broadcasted_iota(I32, (owners, 256), 1)
    digits = jnp.where(
        lane == 127,
        lax.shift_right_logical(count, 7),
        jnp.where(lane == 255, count & 127, 0),
    )
    total = total + dot(last_group, digits.astype(F32).astype(BF))
    req_ref[...] = total[:, :128].astype(I32) * 128 + total[:, 128:].astype(I32)


def route(ids, row_bits, owners):
    return pl.pallas_call(
        functools.partial(route_kernel, row_bits, owners),
        out_shape=(
            jax.ShapeDtypeStruct(ids.shape, I32),
            jax.ShapeDtypeStruct((owners * (REQ // 128), 128), I32),
        ),
        in_specs=[VM],
        out_specs=(VM, VM),
        compiler_params=params(16),
        name="route",
    )(ids)


def lookup_kernel(asked_ref, table_ref, out_ref, wide_ref, row_ref):
    block_rows = table_ref.shape[0]
    owners = asked_ref.shape[0]
    step = 512

    def widen(i, _):
        at = pl.ds(pl.multiple_of(i * step, step), step)
        wide_ref[at, :] = table_ref[at, :].astype(F32)
        return 0

    lax.fori_loop(0, block_rows // step, widen, 0)

    def one(d, _):
        count = asked_ref[d, REQ - 1]

        def eight(i, _):
            base = pl.multiple_of(i * 8, 8)
            for k in range(8):
                row_ref[pl.ds(base + k, 1), :] = wide_ref[pl.ds(asked_ref[d, base + k], 1), :]
            return 0

        lax.fori_loop(0, (count + 7) // 8, eight, 0)
        out_ref[d] = row_ref[...].astype(BF)
        return 0

    lax.fori_loop(0, owners, one, 0)


def lookup(asked, table):
    owners = asked.shape[0]
    return pl.pallas_call(
        lookup_kernel,
        out_shape=jax.ShapeDtypeStruct((owners, CAP, table.shape[1]), BF),
        in_specs=[SM, VM],
        out_specs=VM,
        scratch_shapes=[
            pltpu.VMEM(table.shape, F32),
            pltpu.VMEM((CAP, table.shape[1]), F32),
        ],
        compiler_params=params(24),
        name="lookup",
    )(asked, table)


def unpermute_kernel(slot_ref, got_ref, out_ref, wide_ref, row_ref):
    total = got_ref.shape[0]
    count = out_ref.shape[0]
    step = CAP * 2
    block = row_ref.shape[0]

    def widen(i, _):
        at = pl.ds(pl.multiple_of(i * step, step), step)
        wide_ref[at, :] = got_ref[at, :].astype(F32)
        return 0

    lax.fori_loop(0, total // step, widen, 0)

    def chunk(j, _):
        def eight(i, _):
            base = pl.multiple_of(i * 16, 16)
            for k in range(16):
                row_ref[pl.ds(base + k, 1), :] = wide_ref[pl.ds(slot_ref[j, base + k], 1), :]
            return 0

        lax.fori_loop(0, block // 16, eight, 0)
        out_ref[pl.ds(pl.multiple_of(j * block, block), block), :] = row_ref[...].astype(BF)
        return 0

    lax.fori_loop(0, count // block, chunk, 0)


def unpermute(slots, got):
    rows, width = slots.shape
    return pl.pallas_call(
        unpermute_kernel,
        out_shape=jax.ShapeDtypeStruct((rows * width, got.shape[1]), BF),
        in_specs=[SM, VM],
        out_specs=VM,
        scratch_shapes=[pltpu.VMEM(got.shape, F32), pltpu.VMEM((width, got.shape[1]), F32)],
        compiler_params=params(16),
        name="unpermute",
    )(slots, got)


def attend_quarter(q, length, qkv_ref, out_ref, where, s_ref, v_ref):
    n = s_ref.shape[1]
    full = jnp.minimum(q, length // n)
    some = jnp.minimum(q + 1, (length + n - 1) // n)
    lane = lax.broadcasted_iota(I32, (n, 128), 1)
    rows = pl.ds(pl.multiple_of(q * n, n), n)
    row_pos = q * n + lax.broadcasted_iota(I32, (n, n), 0)
    limit = jnp.minimum(row_pos + 1, length)
    for pair in range(2):
        qp = qkv_ref[rows, pair * 128 : pair * 128 + 128]
        halves = []
        for h in range(2):
            qh = jnp.where((lane < 64) == (h == 0), qp, jnp.zeros_like(qp))

            def block(j, masked):
                at = pl.ds(pl.multiple_of(j * n, n), n)
                s = dot_t(qh, qkv_ref[at, 256 + pair * 128 : 384 + pair * 128]) * (0.125 * LOG2E)
                if masked:
                    col = j * n + lax.broadcasted_iota(I32, (n, n), 1)
                    s = jnp.where(col < limit, s, -1e30)
                s_ref[j] = s
                part = jnp.maximum(
                    jnp.maximum(s[:, 0:128], s[:, 128:256]), jnp.maximum(s[:, 256:384], s[:, 384:512])
                )
                return part

            m = jnp.full((n, 128), -1e30, F32)
            m = lax.fori_loop(0, full, lambda j, m: jnp.maximum(m, block(j, False)), m)
            m = lax.fori_loop(full, some, lambda j, m: jnp.maximum(m, block(j, True)), m)
            top = jnp.max(m, axis=1, keepdims=True)

            def weigh(j, acc):
                at = pl.ds(pl.multiple_of(j * n, n), n)
                p = jnp.exp2(s_ref[j] - top).astype(BF)
                return acc + dot(p, v_ref[pair, at, :])

            acc = lax.fori_loop(0, some, weigh, jnp.zeros((n, 256), F32))
            halves.append(acc[:, :128] / acc[:, 128:])
        out_ref[where, :, pair * 128 : pair * 128 + 128] = jnp.where(
            lane < 64, halves[0], halves[1]
        ).astype(BF)


def fill_values(qkv_ref, v_ref):
    for pair in range(2):
        v_ref[pair, :, 0:128] = qkv_ref[:, 512 + pair * 128 : 640 + pair * 128]
        v_ref[pair, :, 128:256] = jnp.ones((v_ref.shape[1], 128), BF)


def first_kernel(
    meta_ref, s0, s1, s2, s3, gain_ref, w_ref, qkv_ref, att_ref, res_ref, own_w_ref, s_ref, v_ref
):
    c = meta_ref[0]
    length = meta_ref[1]
    n = s_ref.shape[1]
    g = lax.rem(c, 2)
    mate = c + 1 - 2 * g
    slices = ((s0, c), (s1, mate), (s2, 3 - c), (s3, 3 - mate))

    def project(q, keep):
        rows = pl.ds(pl.multiple_of(q * n, n), n)
        wide = [ref[rows, :].astype(F32) for ref, _ in slices]
        square = sum(x * x for x in wide)
        scale = lax.rsqrt(jnp.sum(square, axis=1, keepdims=True) * (1.0 / D) + 1e-06)
        for x, (ref, i) in zip(wide, slices):
            lanes = pl.ds(pl.multiple_of(i * 128, 128), 128)
            if keep is not None:
                res_ref[keep, :, lanes] = ref[rows, :]
        normed = jnp.concatenate(
            [
                (x * scale * gain_ref[pl.ds(i, 1), :]).astype(BF)
                for x, (_, i) in zip(wide, slices)
            ],
            axis=1,
        )
        for k in range(3):
            part = slice(k * 256, k * 256 + 256)
            qkv_ref[rows, part] = dot(normed, own_w_ref[:, part]).astype(BF)

    for at, (_, i) in enumerate(slices):
        for k in range(3):
            lanes = pl.ds(pl.multiple_of(k * D + g * 256, 256), 256)
            own_w_ref[at * 128 : at * 128 + 128, k * 256 : k * 256 + 256] = w_ref[
                pl.ds(pl.multiple_of(i * 128, 128), 128), lanes
            ]
    project(3 - c, 0)
    project(c, 1)
    project(3 - mate, None)
    project(mate, None)
    fill_values(qkv_ref, v_ref)
    for where in range(2):
        q = 3 - mate if where == 0 else mate
        attend_quarter(q, length, qkv_ref, att_ref, where, s_ref, v_ref)


def second_kernel(meta_ref, qkv_ref, att_ref, s_ref, v_ref):
    c = meta_ref[0]
    fill_values(qkv_ref, v_ref)
    for where in range(2):
        q = 3 - c if where == 0 else c
        attend_quarter(q, meta_ref[1], qkv_ref, att_ref, where, s_ref, v_ref)


def first(meta, slices, gain, w_qkv, quarter):
    length = slices[0].shape[0]
    return pl.pallas_call(
        first_kernel,
        out_shape=(
            jax.ShapeDtypeStruct((length, 768), BF),
            jax.ShapeDtypeStruct((2, quarter, 256), BF),
            jax.ShapeDtypeStruct((2, quarter, D), BF),
        ),
        in_specs=[SM] + [VM] * 6,
        out_specs=(VM, VM, VM),
        scratch_shapes=[
            pltpu.VMEM((D, 768), BF),
            pltpu.VMEM((length // quarter, quarter, quarter), F32),
            pltpu.VMEM((2, length, 256), BF),
        ],
        compiler_params=params(40),
        name="project_attend",
    )(meta, *slices, gain, w_qkv)


def second(meta, qkv, quarter):
    length = qkv.shape[0]
    return pl.pallas_call(
        second_kernel,
        out_shape=jax.ShapeDtypeStruct((2, quarter, 256), BF),
        in_specs=[SM, VM],
        out_specs=VM,
        scratch_shapes=[
            pltpu.VMEM((length // quarter, quarter, quarter), F32),
            pltpu.VMEM((2, length, 256), BF),
        ],
        compiler_params=params(32),
        name="attend",
    )(meta, qkv)


def mlp_kernel(meta_ref, own_ref, other_ref, res_ref, wo_ref, gain_ref, wi_ref, wd_ref, out_ref):
    g = lax.rem(meta_ref[0], 2)
    hidden = (
        res_ref[...].astype(F32) + dot(own_ref[...], wo_ref[g]) + dot(other_ref[...], wo_ref[1 - g])
    ).astype(BF)
    hidden = hidden.astype(F32)
    scale = lax.rsqrt(jnp.mean(hidden * hidden, axis=1, keepdims=True) + 1e-06)
    normed = (hidden * scale * gain_ref[...]).astype(BF)
    acc = hidden
    step = 512
    for k in range(FF // step):
        gate = dot(normed, wi_ref[:, k * step : k * step + step])
        up = dot(normed, wi_ref[:, FF + k * step : FF + k * step + step])
        half = 0.5 * gate
        act = ((half + half * jnp.tanh(half)) * up).astype(BF)
        acc = acc + dot(act, wd_ref[k * step : k * step + step, :])
    out_ref[...] = acc.astype(BF)


def mlp(meta, own, other, res, w_out, gain, w_in, w_down):
    return pl.pallas_call(
        mlp_kernel,
        out_shape=jax.ShapeDtypeStruct(res.shape, BF),
        in_specs=[SM] + [VM] * 7,
        out_specs=VM,
        compiler_params=params(24),
        name="mlp",
    )(meta, own, other, res, w_out, gain, w_in, w_down)


def exchange(x, pairs):
    return lax.ppermute(x, "cols", pairs)


def local(token_ids, lengths, table, attn_gain, w_qkv, w_out, mlp_gain, w_in, w_down):
    batch_dev, quarter = token_ids.shape
    owners = lax.axis_size("rows")
    col_count = lax.axis_size("cols")
    c = lax.axis_index("cols")
    h = c // 2
    meta = jnp.stack([c, lax.dynamic_index_in_dim(lengths, h, 0, False)]).astype(I32)
    row_bits = (table.shape[0] - 1).bit_length()

    copies = jnp.broadcast_to(token_ids, (col_count, *token_ids.shape))
    ids = lax.all_to_all(copies, "cols", split_axis=0, concat_axis=0, tiled=True)
    ids = jnp.transpose(ids, (1, 0, 2)).reshape(batch_dev * col_count, quarter)
    slots, requests = route(ids, row_bits, owners)
    asked = lax.all_to_all(
        requests.reshape(owners, REQ), "rows", split_axis=0, concat_axis=0, tiled=True
    )
    looked = lookup(asked, table)
    got = lax.all_to_all(looked, "rows", split_axis=0, concat_axis=0, tiled=True)
    got = got.reshape(owners * CAP, table.shape[1])
    slots = slots.reshape(batch_dev, col_count, quarter)
    theirs = unpermute(lax.dynamic_index_in_dim(slots, 1 - h, 0, False), got)
    mine = unpermute(lax.dynamic_index_in_dim(slots, h, 0, False), got)
    crossed = exchange(theirs, CROSS)
    swapped = exchange(mine, SWAP)
    relayed = exchange(crossed, SWAP)

    qkv, att_mate, res = first(
        meta, (mine, swapped, crossed, relayed), attn_gain.reshape(4, 128), w_qkv, quarter
    )
    other_0 = exchange(att_mate[0], SWAP)
    other_1 = exchange(att_mate[1], SWAP)
    att = second(meta, qkv, quarter)
    halves = w_out.reshape(2, 256, D)
    gain = mlp_gain.reshape(1, D)
    sent = mlp(meta, att[0], other_0, res[0], halves, gain, w_in, w_down)
    came = exchange(sent, CROSS)
    kept = mlp(meta, att[1], other_1, res[1], halves, gain, w_in, w_down)
    mine_first = h == 0
    return jnp.stack([jnp.where(mine_first, kept, came), jnp.where(mine_first, came, kept)])


def solution(mesh):
    in_specs = (P("rows", "cols"), P("rows"), P("rows", "cols"), P(), P(), P(), P(), P(), P())
    out_specs = P("rows", "cols", None)
    return jax.shard_map(local, mesh=mesh, in_specs=in_specs, out_specs=out_specs, check_vma=False)
```

```python
import functools

import jax
import jax.numpy as jnp
from jax import lax
from jax.experimental import pallas as pl
from jax.experimental.pallas import tpu as pltpu
from jax.sharding import PartitionSpec as P

D = 512
FF = 2048
CAP = 344
REQ = 384
LOG2E = 1.4426950408889634
SWAP = [(0, 1), (1, 0), (2, 3), (3, 2)]
CROSS = [(0, 3), (3, 0), (1, 2), (2, 1)]
VM = pl.BlockSpec(memory_space=pltpu.VMEM)
SM = pl.BlockSpec(memory_space=pltpu.SMEM)
HB = pl.BlockSpec(memory_space=pl.ANY)
F32 = jnp.float32
BF = jnp.bfloat16
I32 = jnp.int32


def dot(a, b):
    return lax.dot_general(a, b, (((1,), (0,)), ((), ())), preferred_element_type=F32)


def dot_t(a, b):
    return lax.dot_general(a, b, (((1,), (1,)), ((), ())), preferred_element_type=F32)


def params(mib):
    return pltpu.CompilerParams(vmem_limit_bytes=mib * 1024 * 1024)


def route_kernel(row_bits, owners, ids_ref, slot_ref, req_ref):
    rows, width = ids_ref.shape
    parts = REQ // 128
    upper = (
        lax.broadcasted_iota(I32, (width, width), 0) < lax.broadcasted_iota(I32, (width, width), 1)
    ).astype(BF)
    owner_iota = lax.broadcasted_iota(I32, (owners, width), 0)
    group_iota = lax.broadcasted_iota(I32, (owners * parts, width), 0)
    lane_iota = lax.broadcasted_iota(I32, (128, width), 0)
    carry = jnp.zeros((owners, 1), F32)
    total = jnp.zeros((owners * parts, 256), F32)
    for r in range(rows):
        ids = ids_ref[r : r + 1, :]
        owner = lax.shift_right_logical(ids, row_bits)
        offset = ids & ((1 << row_bits) - 1)
        hot = (owner_iota == owner).astype(F32)
        before = dot(hot.astype(BF), upper) + carry
        rank = jnp.sum(hot * before, axis=0, keepdims=True).astype(I32)
        carry = carry + jnp.sum(hot, axis=1, keepdims=True)
        slot_ref[r : r + 1, :] = owner * CAP + rank
        group = owner * parts + lax.shift_right_logical(rank, 7)
        in_group = (group_iota == group).astype(BF)
        at_lane = lane_iota == (rank & 127)
        high = jnp.where(at_lane, lax.shift_right_logical(offset, 7), 0).astype(F32).astype(BF)
        low = jnp.where(at_lane, offset & 127, 0).astype(F32).astype(BF)
        total = total + dot_t(in_group, jnp.concatenate([high, low], axis=0))
    count = carry.astype(I32)
    last_group = (
        lax.broadcasted_iota(I32, (owners * parts, owners), 0)
        == lax.broadcasted_iota(I32, (owners * parts, owners), 1) * parts + parts - 1
    ).astype(BF)
    lane = lax.broadcasted_iota(I32, (owners, 256), 1)
    digits = jnp.where(
        lane == 127,
        lax.shift_right_logical(count, 7),
        jnp.where(lane == 255, count & 127, 0),
    )
    total = total + dot(last_group, digits.astype(F32).astype(BF))
    req_ref[...] = total[:, :128].astype(I32) * 128 + total[:, 128:].astype(I32)


def route(ids, row_bits, owners):
    return pl.pallas_call(
        functools.partial(route_kernel, row_bits, owners),
        out_shape=(
            jax.ShapeDtypeStruct(ids.shape, I32),
            jax.ShapeDtypeStruct((owners * (REQ // 128), 128), I32),
        ),
        in_specs=[VM],
        out_specs=(VM, VM),
        compiler_params=params(16),
        name="route",
    )(ids)


def lookup_kernel(asked_ref, table_ref, out_ref, part_ref, wide_ref, row_ref, send_ref, in_sem, out_sem):
    step = part_ref.shape[1]
    chunks = part_ref.shape[0]
    owners = out_ref.shape[0]

    def fetch(i):
        return pltpu.make_async_copy(
            table_ref.at[pl.ds(i * step, step)], part_ref.at[i], in_sem.at[i]
        )

    def store(d):
        return pltpu.make_async_copy(send_ref.at[d], out_ref.at[d], out_sem.at[d])

    for i in range(chunks):
        fetch(i).start()
    for i in range(chunks):
        fetch(i).wait()
        piece = 512

        def widen(j, _):
            at = pl.multiple_of(j * piece, piece)
            wide_ref[pl.ds(i * step + at, piece), :] = part_ref[i, pl.ds(at, piece), :].astype(F32)
            return 0

        lax.fori_loop(0, step // piece, widen, 0)

    def one(d, _):
        start = d * REQ
        count = asked_ref[start + REQ - 1]

        def some(i, _):
            base = pl.multiple_of(i * 8, 8)
            first = start + base
            for k in range(8):
                row_ref[pl.ds(base + k, 1), :] = wide_ref[pl.ds(asked_ref[first + k], 1), :]
            return 0

        lax.fori_loop(0, lax.shift_right_logical(count + 7, 3), some, 0)
        send_ref[d] = row_ref[...].astype(BF)
        store(d).start()
        return 0

    lax.fori_loop(0, owners, one, 0)

    def finish(d, _):
        store(d).wait()
        return 0

    lax.fori_loop(0, owners, finish, 0)


def lookup(asked, table, owners):
    rows, width = table.shape
    chunks = 8
    return pl.pallas_call(
        lookup_kernel,
        out_shape=jax.ShapeDtypeStruct((owners, CAP, width), BF),
        in_specs=[SM, HB],
        out_specs=HB,
        scratch_shapes=[
            pltpu.VMEM((chunks, rows // chunks, width), BF),
            pltpu.VMEM((rows, width), F32),
            pltpu.VMEM((CAP, width), F32),
            pltpu.VMEM((owners, CAP, width), BF),
            pltpu.SemaphoreType.DMA((chunks,)),
            pltpu.SemaphoreType.DMA((owners,)),
        ],
        compiler_params=params(24),
        name="lookup",
    )(asked, table)


def pick(slot_ref, start, wide_ref, row_ref, out_ref):
    block = row_ref.shape[0]

    def chunk(j, _):
        first = start + j * block

        def some(i, _):
            base = pl.multiple_of(i * 8, 8)
            at = first + base
            for k in range(8):
                row_ref[pl.ds(base + k, 1), :] = wide_ref[pl.ds(slot_ref[at + k], 1), :]
            return 0

        lax.fori_loop(0, block // 8, some, 0)
        out_ref[pl.ds(pl.multiple_of(j * block, block), block), :] = row_ref[...].astype(BF)
        return 0

    lax.fori_loop(0, out_ref.shape[0] // block, chunk, 0)


def pick_first_kernel(meta_ref, slot_ref, got_ref, out_ref, wide_ref, part_ref, row_ref, sem):
    chunks, step, _ = part_ref.shape

    def fetch(i):
        return pltpu.make_async_copy(got_ref.at[pl.ds(i * step, step)], part_ref.at[i], sem.at[i])

    for i in range(chunks):
        fetch(i).start()
    for i in range(chunks):
        fetch(i).wait()
        wide_ref[pl.ds(i * step, step), :] = part_ref[i].astype(F32)
    pick(slot_ref, meta_ref[2], wide_ref, row_ref, out_ref)


def pick_more_kernel(where, meta_ref, slot_ref, wide_ref, *refs):
    outs, row_ref = refs[:-1], refs[-1]
    for (of, late), out_ref in zip(where, outs):
        start = meta_ref[2 + of] + late * out_ref.shape[0]
        pick(slot_ref, start, wide_ref, row_ref, out_ref)


def pick_first(meta, slots, got, half):
    rows, width = got.shape
    chunks = 8
    return pl.pallas_call(
        pick_first_kernel,
        out_shape=(
            jax.ShapeDtypeStruct((half, width), BF),
            jax.ShapeDtypeStruct((rows, width), F32),
        ),
        in_specs=[SM, SM, HB],
        out_specs=(VM, VM),
        scratch_shapes=[
            pltpu.VMEM((chunks, rows // chunks, width), BF),
            pltpu.VMEM((512, width), F32),
            pltpu.SemaphoreType.DMA((chunks,)),
        ],
        compiler_params=params(16),
        name="pick_first",
    )(meta, slots, got)


def pick_more(meta, slots, wide, half, where):
    width = wide.shape[1]
    return pl.pallas_call(
        functools.partial(pick_more_kernel, where),
        out_shape=[jax.ShapeDtypeStruct((half, width), BF) for _ in where],
        in_specs=[SM, SM, VM],
        out_specs=[VM for _ in where],
        scratch_shapes=[pltpu.VMEM((512, width), F32)],
        compiler_params=params(16),
        name="pick_more",
    )(meta, slots, wide)


def project(c, slices, gain_ref, w_ref, norm_ref, k_ref, v_ref, res_ref, mine):
    n = norm_ref.shape[1]
    mate = lax.bitwise_xor(c, 1)
    order = (c, mate, 3 - c, 3 - mate)
    for b in range(2):
        rows = slice(b * n, b * n + n)
        wide = [ref[rows, :].astype(F32) for ref in slices]
        square = sum(x * x for x in wide)
        scale = lax.rsqrt(jnp.sum(square, axis=1, keepdims=True) * (1.0 / D) + 1e-06)
        normed = jnp.concatenate(
            [(x * scale * gain_ref[pl.ds(i, 1), :]).astype(BF) for x, i in zip(wide, order)],
            axis=1,
        )
        norm_ref[b] = normed
        keys = dot(normed, w_ref[:, D : 2 * D]).astype(BF)
        values = dot(normed, w_ref[:, 2 * D :]).astype(BF)
        for pair in range(4):
            k_ref[pair, rows, :] = keys[:, pair * 128 : pair * 128 + 128]
            v_ref[pair, rows, 0:128] = values[:, pair * 128 : pair * 128 + 128]
            v_ref[pair, rows, 128:256] = jnp.ones((n, 128), BF)
    own = pl.ds(pl.multiple_of(mine * n, n), n)
    for ref, i in zip(slices, order):
        res_ref[:, pl.ds(pl.multiple_of(i * 128, 128), 128)] = ref[own, :]
    return (dot(norm_ref[mine], w_ref[:, 0:D]) * (0.125 * LOG2E)).astype(BF)


def attend(quarter, length, q, q_ref, keys, values, s_ref, out_ref):
    size = s_ref.shape[2]
    for pair in range(4):
        q_ref[pair] = q[:, pair * 128 : pair * 128 + 128]
    subs = q_ref.shape[1] // size
    per_half = keys[0].shape[1] // size
    lane = lax.broadcasted_iota(I32, (size, 128), 1)
    row = lax.broadcasted_iota(I32, (size, size), 0)
    col = lax.broadcasted_iota(I32, (size, size), 1)

    def item(it, _):
        pair = lax.shift_right_logical(it, 1)
        sub = it & 1
        rows = pl.ds(pl.multiple_of(sub * size, size), size)
        block = quarter * subs + sub
        need = jnp.minimum(block + 1, lax.shift_right_logical(length + size - 1, 8))

        def body(n):
            qp = q_ref[pair, rows, :]
            limit = jnp.minimum(block * size + row + 1, length) - (n - 1) * size
            tops = []
            for head in range(2):
                qh = jnp.where((lane < 64) == (head == 0), qp, jnp.zeros_like(qp))
                m = None
                for j in range(n):
                    at = slice(j % per_half * size, j % per_half * size + size)
                    s = dot_t(qh, keys[j // per_half][pair, at, :])
                    if j == n - 1:
                        s = jnp.where(col < limit, s, -1e30)
                    s_ref[head, j] = s
                    t = jnp.maximum(s[:, 0:128], s[:, 128:256])
                    m = t if m is None else jnp.maximum(m, t)
                tops.append(jnp.max(m, axis=1, keepdims=True))
            outs = []
            for head in range(2):
                acc = None
                for j in range(n):
                    at = slice(j % per_half * size, j % per_half * size + size)
                    p = jnp.exp2(s_ref[head, j] - tops[head]).astype(BF)
                    d = dot(p, values[j // per_half][pair, at, :])
                    acc = d if acc is None else acc + d
                outs.append(acc[:, :128] / acc[:, 128:])
            out_ref[pair, rows, :] = jnp.where(lane < 64, outs[0], outs[1]).astype(BF)

        for n in range(1, s_ref.shape[1] + 1):
            pl.when(need == n)(functools.partial(body, n))
        return 0

    lax.fori_loop(0, 4 * subs, item, 0)


def early_kernel(
    meta_ref, s0, s1, s2, s3, gain_ref, w_ref,
    k_ref, v_ref, own_w_ref, att_ref, res_ref, norm_ref, q_ref, s_ref,
):
    c = meta_ref[0]
    mate = lax.bitwise_xor(c, 1)
    for at, i in enumerate((c, mate, 3 - c, 3 - mate)):
        own_w_ref[at * 128 : at * 128 + 128, :] = w_ref[pl.ds(pl.multiple_of(i * 128, 128), 128), :]
    quarter = jnp.minimum(c, 3 - c)
    q = project(c, (s0, s1, s2, s3), gain_ref, own_w_ref, norm_ref, k_ref, v_ref, res_ref, quarter)
    attend(quarter, meta_ref[1], q, q_ref, (k_ref,), (v_ref,), s_ref, att_ref)


def late_kernel(
    meta_ref, s0, s1, s2, s3, gain_ref, own_w_ref, k0_ref, v0_ref,
    att_ref, res_ref, norm_ref, q_ref, s_ref, k_ref, v_ref,
):
    c = meta_ref[0]
    quarter = jnp.maximum(c, 3 - c)
    q = project(
        c, (s0, s1, s2, s3), gain_ref, own_w_ref, norm_ref, k_ref, v_ref, res_ref, quarter - 2
    )
    attend(quarter, meta_ref[1], q, q_ref, (k0_ref, k_ref), (v0_ref, v_ref), s_ref, att_ref)


def attention_scratch(quarter, blocks):
    return [
        pltpu.VMEM((2, quarter, D), BF),
        pltpu.VMEM((4, quarter, 128), BF),
        pltpu.VMEM((2, blocks, 256, 256), F32),
    ]


def early(meta, slices, gain, w_qkv, quarter):
    half = 2 * quarter
    return pl.pallas_call(
        early_kernel,
        out_shape=(
            jax.ShapeDtypeStruct((4, half, 128), BF),
            jax.ShapeDtypeStruct((4, half, 256), BF),
            jax.ShapeDtypeStruct(w_qkv.shape, BF),
            jax.ShapeDtypeStruct((4, quarter, 128), BF),
            jax.ShapeDtypeStruct((quarter, D), BF),
        ),
        in_specs=[SM] + [VM] * 6,
        out_specs=(VM,) * 5,
        scratch_shapes=attention_scratch(quarter, half // 256),
        compiler_params=params(24),
        name="early",
    )(meta, *slices, gain, w_qkv)


def late(meta, slices, gain, own_w, keys, values, quarter):
    half = 2 * quarter
    return pl.pallas_call(
        late_kernel,
        out_shape=(
            jax.ShapeDtypeStruct((4, quarter, 128), BF),
            jax.ShapeDtypeStruct((quarter, D), BF),
        ),
        in_specs=[SM] + [VM] * 8,
        out_specs=(VM, VM),
        scratch_shapes=attention_scratch(quarter, 2 * half // 256)
        + [pltpu.VMEM((4, half, 128), BF), pltpu.VMEM((4, half, 256), BF)],
        compiler_params=params(24),
        name="late",
    )(meta, *slices, gain, own_w, keys, values)


def mlp_kernel(start, att_ref, res_ref, wo_ref, gain_ref, wi_ref, wd_ref, out_ref):
    rows = slice(start, start + out_ref.shape[0])
    attended = jnp.concatenate([att_ref[pair, rows, :] for pair in range(4)], axis=1)
    hidden = (res_ref[rows, :].astype(F32) + dot(attended, wo_ref[...])).astype(BF)
    hidden = hidden.astype(F32)
    scale = lax.rsqrt(jnp.mean(hidden * hidden, axis=1, keepdims=True) + 1e-06)
    normed = (hidden * scale * gain_ref[...]).astype(BF)
    acc = hidden
    step = 512
    for k in range(FF // step):
        gate = dot(normed, wi_ref[:, k * step : k * step + step])
        up = dot(normed, wi_ref[:, FF + k * step : FF + k * step + step])
        half = 0.5 * gate
        act = ((half + half * jnp.tanh(half)) * up).astype(BF)
        acc = acc + dot(act, wd_ref[k * step : k * step + step, :])
    out_ref[...] = acc.astype(BF)


def mlp(att, res, weights, start, count):
    return pl.pallas_call(
        functools.partial(mlp_kernel, start),
        out_shape=jax.ShapeDtypeStruct((count, D), BF),
        in_specs=[VM] * 6,
        out_specs=VM,
        compiler_params=params(20),
        name="mlp",
    )(att, res, *weights)


def exchange(x, pairs):
    return lax.ppermute(x, "cols", pairs)


def local(token_ids, lengths, table, attn_gain, w_qkv, w_out, mlp_gain, w_in, w_down):
    batch_dev, quarter = token_ids.shape
    owners = lax.axis_size("rows")
    col_count = lax.axis_size("cols")
    half = 2 * quarter
    length = col_count * quarter
    c = lax.axis_index("cols")
    h = c // 2
    row_bits = (table.shape[0] - 1).bit_length()
    meta = jnp.stack([c, jnp.where(h == 0, lengths[0], lengths[1]), (1 - h) * length, h * length])
    meta = meta.astype(I32)

    copies = jnp.broadcast_to(token_ids, (col_count, *token_ids.shape))
    ids = lax.all_to_all(copies, "cols", split_axis=0, concat_axis=0, tiled=True)
    ids = jnp.transpose(ids, (1, 0, 2)).reshape(batch_dev * col_count, quarter)
    slots, requests = route(ids, row_bits, owners)
    asked = lax.all_to_all(
        requests.reshape(owners, REQ), "rows", split_axis=0, concat_axis=0, tiled=True
    )
    looked = lookup(asked.reshape(-1), table, owners)
    got = lax.all_to_all(looked, "rows", split_axis=0, concat_axis=0, tiled=True)
    got = got.reshape(owners * CAP, table.shape[1])
    slots = slots.reshape(-1)

    theirs_0, wide = pick_first(meta, slots, got, half)
    crossed_0 = exchange(theirs_0, CROSS)
    mine_0, theirs_1 = pick_more(meta, slots, wide, half, ((1, 0), (0, 1)))
    swapped_0 = exchange(mine_0, SWAP)
    crossed_1 = exchange(theirs_1, CROSS)
    (mine_1,) = pick_more(meta, slots, wide, half, ((1, 1),))
    relayed_0 = exchange(crossed_0, SWAP)
    swapped_1 = exchange(mine_1, SWAP)
    relayed_1 = exchange(crossed_1, SWAP)

    gain = attn_gain.reshape(col_count, -1)
    keys, values, own_w, att_0, res_0 = early(
        meta, (mine_0, swapped_0, crossed_0, relayed_0), gain, w_qkv, quarter
    )
    weights = (w_out, mlp_gain.reshape(1, -1), w_in, w_down)
    out_0 = mlp(att_0, res_0, weights, 0, quarter)
    came_0 = exchange(out_0, [(2, 1), (3, 0)])
    att_1, res_1 = late(
        meta, (mine_1, swapped_1, crossed_1, relayed_1), gain, own_w, keys, values, quarter
    )
    out_1a = mlp(att_1, res_1, weights, 0, quarter // 2)
    came_1a = exchange(out_1a, [(0, 3), (1, 2)])
    out_1b = mlp(att_1, res_1, weights, quarter // 2, quarter // 2)
    came_1b = exchange(out_1b, [(0, 3), (1, 2)])
    first = h == 0
    halves = []
    for at, own_1, came_1 in ((0, out_1a, came_1a), (quarter // 2, out_1b, came_1b)):
        rows = slice(at, at + quarter // 2)
        own = jnp.where(first, out_0[rows], own_1)
        came = jnp.where(first, came_0[rows], came_1)
        which = lax.broadcasted_iota(I32, (batch_dev, quarter // 2, D), 0)
        halves.append(jnp.where(which == h, own[None], came[None]))
    return jnp.concatenate(halves, axis=1)


def solution(mesh):
    in_specs = (P("rows", "cols"), P("rows"), P("rows", "cols"), P(), P(), P(), P(), P(), P())
    out_specs = P("rows", "cols", None)
    return jax.shard_map(local, mesh=mesh, in_specs=in_specs, out_specs=out_specs, check_vma=False)
```

```python
import functools

import jax
import jax.numpy as jnp
from jax import lax
from jax.experimental import pallas as pl
from jax.experimental.pallas import tpu as pltpu
from jax.sharding import PartitionSpec as P

D = 512
FF = 2048
CAP = 344
REQ = 384
LOG2E = 1.4426950408889634
SWAP = [(0, 1), (1, 0), (2, 3), (3, 2)]
CROSS = [(0, 3), (3, 0), (1, 2), (2, 1)]
VM = pl.BlockSpec(memory_space=pltpu.VMEM)
SM = pl.BlockSpec(memory_space=pltpu.SMEM)
AN = pl.BlockSpec(memory_space=pl.ANY)
F32 = jnp.float32
BF = jnp.bfloat16
I32 = jnp.int32


def dot(a, b):
    return lax.dot_general(a, b, (((1,), (0,)), ((), ())), preferred_element_type=F32)


def dot_t(a, b):
    return lax.dot_general(a, b, (((1,), (1,)), ((), ())), preferred_element_type=F32)


def cost(flops, moved=0):
    return pl.CostEstimate(flops=int(flops), bytes_accessed=int(moved), transcendentals=0)


def params(mib):
    return pltpu.CompilerParams(vmem_limit_bytes=mib * 1024 * 1024)


def route_kernel(row_bits, owners, ids_ref, slot_ref, req_ref):
    rows, width = ids_ref.shape
    parts = REQ // 128
    upper = (
        lax.broadcasted_iota(I32, (width, width), 0) < lax.broadcasted_iota(I32, (width, width), 1)
    ).astype(BF)
    owner_iota = lax.broadcasted_iota(I32, (owners, width), 0)
    group_iota = lax.broadcasted_iota(I32, (owners * parts, width), 0)
    lane_iota = lax.broadcasted_iota(I32, (128, width), 0)
    carry = jnp.zeros((owners, 1), F32)
    total = jnp.zeros((owners * parts, 256), F32)
    for r in range(rows):
        ids = ids_ref[r : r + 1, :]
        owner = lax.shift_right_logical(ids, row_bits)
        offset = ids & ((1 << row_bits) - 1)
        hot = (owner_iota == owner).astype(F32)
        before = dot(hot.astype(BF), upper) + carry
        rank = jnp.sum(hot * before, axis=0, keepdims=True).astype(I32)
        carry = carry + jnp.sum(hot, axis=1, keepdims=True)
        slot_ref[r : r + 1, :] = owner * CAP + rank
        place = rank + 1
        group = owner * parts + lax.shift_right_logical(place, 7)
        in_group = (group_iota == group).astype(BF)
        at_lane = lane_iota == (place & 127)
        high = jnp.where(at_lane, lax.shift_right_logical(offset, 7), 0).astype(F32).astype(BF)
        low = jnp.where(at_lane, offset & 127, 0).astype(F32).astype(BF)
        total = total + dot_t(in_group, jnp.concatenate([high, low], axis=0))
    count = carry.astype(I32)
    first_group = (
        lax.broadcasted_iota(I32, (owners * parts, owners), 0)
        == lax.broadcasted_iota(I32, (owners * parts, owners), 1) * parts
    ).astype(BF)
    lane = lax.broadcasted_iota(I32, (owners, 256), 1)
    digits = jnp.where(
        lane == 0,
        lax.shift_right_logical(count, 7),
        jnp.where(lane == 128, count & 127, 0),
    )
    total = total + dot(first_group, digits.astype(F32).astype(BF))
    req_ref[...] = total[:, :128].astype(I32) * 128 + total[:, 128:].astype(I32)


def route(ids, row_bits, owners):
    return pl.pallas_call(
        functools.partial(route_kernel, row_bits, owners),
        out_shape=(
            jax.ShapeDtypeStruct(ids.shape, I32),
            jax.ShapeDtypeStruct((owners * (REQ // 128), 128), I32),
        ),
        in_specs=[VM],
        out_specs=(VM, VM),
        compiler_params=params(16),
        name="route",
    )(ids)


def lookup_kernel(
    asked_ref, table_ref, out_ref,
    ask_ref, part_ref, wide_ref, row_ref, send_ref, ask_sem, in_sem, out_sem,
):
    owners = out_ref.shape[0]
    chunks, step, _ = part_ref.shape
    batches = 4
    batch = owners // batches

    def ask(i):
        at = pl.ds(i * batch * REQ, batch * REQ)
        return pltpu.make_async_copy(asked_ref.at[at], ask_ref.at[at], ask_sem.at[i])

    def fetch(i):
        return pltpu.make_async_copy(table_ref.at[pl.ds(i * step, step)], part_ref.at[i], in_sem.at[i])

    def store(d):
        return pltpu.make_async_copy(send_ref.at[d], out_ref.at[d], out_sem.at[d])

    for i in range(chunks):
        fetch(i).start()
    for i in range(batches):
        ask(i).start()
    piece = 512
    for i in range(chunks):
        fetch(i).wait()

        def widen(j, _):
            at = pl.multiple_of(j * piece, piece)
            wide_ref[pl.ds(i * step + at, piece), :] = part_ref[i, pl.ds(at, piece), :].astype(F32)
            return 0

        lax.fori_loop(0, step // piece, widen, 0)

    def one(d, _):
        start = d * REQ
        groups = lax.shift_right_logical(ask_ref[start] + 31, 5)

        def some(i, _):
            base = pl.multiple_of(i * 32, 32)
            first = start + base + 1
            for k in range(32):
                row_ref[pl.ds(base + k, 1), :] = wide_ref[pl.ds(ask_ref[first + k], 1), :]
            return 0

        lax.fori_loop(0, groups, some, 0)

        def narrow(i, _):
            at = pl.ds(pl.multiple_of(i * 32, 32), 32)
            send_ref[d, at, :] = row_ref[at, :].astype(BF)
            return 0

        lax.fori_loop(0, jnp.minimum(groups, CAP // 32), narrow, 0)

        @pl.when(groups > CAP // 32)
        def _():
            at = slice(CAP // 32 * 32, CAP)
            send_ref[d, at, :] = row_ref[at, :].astype(BF)

        store(d).start()
        return 0

    for i in range(batches):
        ask(i).wait()
        lax.fori_loop(i * batch, i * batch + batch, one, 0)

    def finish(d, _):
        store(d).wait()
        return 0

    lax.fori_loop(0, owners, finish, 0)


def lookup(asked, table, owners):
    rows, width = table.shape
    chunks = 8
    return pl.pallas_call(
        lookup_kernel,
        out_shape=jax.ShapeDtypeStruct((owners, CAP, width), BF),
        in_specs=[AN, AN],
        out_specs=AN,
        scratch_shapes=[
            pltpu.SMEM((owners * REQ,), I32),
            pltpu.VMEM((chunks, rows // chunks, width), BF),
            pltpu.VMEM((rows, width), F32),
            pltpu.VMEM((352, width), F32),
            pltpu.VMEM((owners, CAP, width), BF),
            pltpu.SemaphoreType.DMA((4,)),
            pltpu.SemaphoreType.DMA((chunks,)),
            pltpu.SemaphoreType.DMA((owners,)),
        ],
        compiler_params=params(62),
        cost_estimate=cost(6e9, 4e6),
        name="lookup",
    )(asked, table)


def slots_of(other, late, meta_ref, slot_ref, here_ref, sem):
    half = here_ref.shape[0]
    history = lax.shift_right_logical(meta_ref[0], 1)
    history = 1 - history if other else history
    start = pl.multiple_of((history * 2 + late) * half, half)
    return pltpu.make_async_copy(slot_ref.at[pl.ds(start, half)], here_ref, sem)


def pick(here_ref, wide_ref, row_ref, out_ref):
    block = row_ref.shape[0]
    for j in range(out_ref.shape[0] // block):

        def some(i, _):
            base = pl.multiple_of(i * 32, 32)
            at = j * block + base
            for k in range(32):
                row_ref[pl.ds(base + k, 1), :] = wide_ref[pl.ds(here_ref[at + k], 1), :]
            return 0

        lax.fori_loop(0, block // 32, some, 0)
        out_ref[j * block : j * block + block, :] = row_ref[...].astype(BF)


def pick_first_kernel(meta_ref, slot_ref, got_ref, out_ref, wide_ref, row_ref, here_ref, sem):
    step = 2 * CAP
    copy = slots_of(True, 0, meta_ref, slot_ref, here_ref, sem)
    copy.start()

    def widen(i, _):
        at = pl.ds(pl.multiple_of(i * step, step), step)
        wide_ref[at, :] = got_ref[at, :].astype(F32)
        return 0

    lax.fori_loop(0, wide_ref.shape[0] // step, widen, 0)
    copy.wait()
    pick(here_ref, wide_ref, row_ref, out_ref)


def pick_more_kernel(
    other, late, meta_ref, slot_ref, wide_ref, after_ref, out_ref, row_ref, here_ref, sem
):
    copy = slots_of(other, late, meta_ref, slot_ref, here_ref, sem)
    copy.start()
    copy.wait()
    pick(here_ref, wide_ref, row_ref, out_ref)


def pick_scratch(half, quarter, width):
    return [
        pltpu.VMEM((quarter, width), F32),
        pltpu.SMEM((half,), I32),
        pltpu.SemaphoreType.DMA,
    ]


def pick_first(meta, slots, got, half, quarter):
    rows, width = got.shape
    return pl.pallas_call(
        pick_first_kernel,
        out_shape=(
            jax.ShapeDtypeStruct((half, width), BF),
            jax.ShapeDtypeStruct((rows, width), F32),
        ),
        in_specs=[SM, AN, VM],
        out_specs=(VM, VM),
        scratch_shapes=pick_scratch(half, quarter, width),
        compiler_params=params(14),
        cost_estimate=cost(3e9, 4e6),
        name="pick_first",
    )(meta, slots, got)


def pick_more(meta, slots, wide, after, half, quarter, other, late):
    width = wide.shape[1]
    return pl.pallas_call(
        functools.partial(pick_more_kernel, other, late),
        out_shape=jax.ShapeDtypeStruct((half, width), BF),
        in_specs=[SM, AN, VM, AN],
        out_specs=VM,
        scratch_shapes=pick_scratch(half, quarter, width),
        compiler_params=params(14),
        cost_estimate=cost(2e9, 4e6),
        name="pick_more",
    )(meta, slots, wide, after)


def project(c, slices, gain_ref, w_ref, norm_ref, k_ref, v_ref, res_ref, mine):
    n = norm_ref.shape[1]
    mate = lax.bitwise_xor(c, 1)
    order = (c, mate, 3 - c, 3 - mate)
    for b in range(2):
        rows = slice(b * n, b * n + n)
        wide = [ref[rows, :].astype(F32) for ref in slices]
        square = sum(x * x for x in wide)
        scale = lax.rsqrt(jnp.sum(square, axis=1, keepdims=True) * (1.0 / D) + 1e-06)
        normed = jnp.concatenate(
            [(x * scale * gain_ref[pl.ds(i, 1), :]).astype(BF) for x, i in zip(wide, order)],
            axis=1,
        )
        norm_ref[b] = normed
        keys = dot(normed, w_ref[:, D : 2 * D]).astype(BF)
        values = dot(normed, w_ref[:, 2 * D :]).astype(BF)
        for pair in range(4):
            k_ref[pair, rows, :] = keys[:, pair * 128 : pair * 128 + 128]
            v_ref[pair, rows, 0:128] = values[:, pair * 128 : pair * 128 + 128]
            v_ref[pair, rows, 128:256] = jnp.ones((n, 128), BF)
    own = pl.ds(pl.multiple_of(mine * n, n), n)
    for ref, i in zip(slices, order):
        res_ref[:, pl.ds(pl.multiple_of(i * 128, 128), 128)] = ref[own, :]
    return (dot(norm_ref[mine], w_ref[:, 0:D]) * (0.125 * LOG2E)).astype(BF)


def keep_queries(q, q_ref):
    for pair in range(4):
        q_ref[pair] = q[:, pair * 128 : pair * 128 + 128]


def attend(quarter, length, q_ref, keys, values, s_ref, out_ref, skip=0):
    size = s_ref.shape[2]
    subs = q_ref.shape[1] // size
    todo = out_ref.shape[1] // size
    per_half = keys[0].shape[1] // size
    lane = lax.broadcasted_iota(I32, (size, 128), 1)
    row = lax.broadcasted_iota(I32, (size, size), 0)
    col = lax.broadcasted_iota(I32, (size, size), 1)

    def item(it, _):
        pair = it & 3
        at_sub = lax.shift_right_logical(it, 2)
        put = pl.ds(pl.multiple_of(at_sub * size, size), size)
        rows = pl.ds(pl.multiple_of((at_sub + skip) * size, size), size)
        block = quarter * subs + at_sub + skip
        need = jnp.minimum(block + 1, lax.shift_right_logical(length + size - 1, 8))

        def body(n):
            qp = q_ref[pair, rows, :]
            limit = jnp.minimum(block * size + row + 1, length) - (n - 1) * size
            tops = []
            for head in range(2):
                qh = jnp.where((lane < 64) == (head == 0), qp, jnp.zeros_like(qp))
                m = None
                for j in range(n):
                    at = slice(j % per_half * size, j % per_half * size + size)
                    s = dot_t(qh, keys[j // per_half][pair, at, :])
                    if j == n - 1:
                        s = jnp.where(col < limit, s, -1e30)
                    s_ref[head, j] = s
                    t = jnp.maximum(s[:, 0:128], s[:, 128:256])
                    m = t if m is None else jnp.maximum(m, t)
                tops.append(jnp.max(m, axis=1, keepdims=True))
            outs = []
            for head in range(2):
                acc = None
                for j in range(n):
                    at = slice(j % per_half * size, j % per_half * size + size)
                    p = jnp.exp2(s_ref[head, j] - tops[head]).astype(BF)
                    d = dot(p, values[j // per_half][pair, at, :])
                    acc = d if acc is None else acc + d
                outs.append(acc[:, :128] / acc[:, 128:])
            out_ref[pair, put, :] = jnp.where(lane < 64, outs[0], outs[1]).astype(BF)

        for n in range(1, s_ref.shape[1] + 1):
            pl.when(need == n)(functools.partial(body, n))
        return 0

    lax.fori_loop(0, 4 * todo, item, 0)


def early_kernel(
    meta_ref, s0, s1, s2, s3, gain_ref, w_ref,
    k_ref, v_ref, own_w_ref, att_ref, res_ref, norm_ref, q_ref, s_ref,
):
    c = meta_ref[0]
    mate = lax.bitwise_xor(c, 1)
    for at, i in enumerate((c, mate, 3 - c, 3 - mate)):
        own_w_ref[at * 128 : at * 128 + 128, :] = w_ref[pl.ds(pl.multiple_of(i * 128, 128), 128), :]
    quarter = jnp.minimum(c, 3 - c)
    q = project(c, (s0, s1, s2, s3), gain_ref, own_w_ref, norm_ref, k_ref, v_ref, res_ref, quarter)
    keep_queries(q, q_ref)
    attend(quarter, meta_ref[1], q_ref, (k_ref,), (v_ref,), s_ref, att_ref)


def late_kernel(
    meta_ref, s0, s1, s2, s3, gain_ref, own_w_ref, k0_ref, v0_ref,
    k_ref, v_ref, q_ref, att_ref, res_ref, norm_ref, s_ref,
):
    c = meta_ref[0]
    quarter = jnp.maximum(c, 3 - c)
    q = project(
        c, (s0, s1, s2, s3), gain_ref, own_w_ref, norm_ref, k_ref, v_ref, res_ref, quarter - 2
    )
    keep_queries(q, q_ref)
    attend(quarter, meta_ref[1], q_ref, (k0_ref, k_ref), (v0_ref, v_ref), s_ref, att_ref)


def last_kernel(meta_ref, q_ref, k0_ref, v0_ref, k_ref, v_ref, after_ref, att_ref, s_ref):
    c = meta_ref[0]
    quarter = jnp.maximum(c, 3 - c)
    attend(quarter, meta_ref[1], q_ref, (k0_ref, k_ref), (v0_ref, v_ref), s_ref, att_ref, 1)


def early(meta, slices, gain, w_qkv, quarter):
    half = 2 * quarter
    return pl.pallas_call(
        early_kernel,
        out_shape=(
            jax.ShapeDtypeStruct((4, half, 128), BF),
            jax.ShapeDtypeStruct((4, half, 256), BF),
            jax.ShapeDtypeStruct(w_qkv.shape, BF),
            jax.ShapeDtypeStruct((4, quarter, 128), BF),
            jax.ShapeDtypeStruct((quarter, D), BF),
        ),
        in_specs=[SM] + [VM] * 6,
        out_specs=(VM,) * 5,
        scratch_shapes=[
            pltpu.VMEM((2, quarter, D), BF),
            pltpu.VMEM((4, quarter, 128), BF),
            pltpu.VMEM((2, half // 256, 256, 256), F32),
        ],
        compiler_params=params(20),
        cost_estimate=cost(7e9, 6e6),
        name="early",
    )(meta, *slices, gain, w_qkv)


def late(meta, slices, gain, own_w, keys, values, quarter):
    half = 2 * quarter
    return pl.pallas_call(
        late_kernel,
        out_shape=(
            jax.ShapeDtypeStruct((4, half, 128), BF),
            jax.ShapeDtypeStruct((4, half, 256), BF),
            jax.ShapeDtypeStruct((4, quarter, 128), BF),
            jax.ShapeDtypeStruct((4, quarter // 2, 128), BF),
            jax.ShapeDtypeStruct((quarter, D), BF),
        ),
        in_specs=[SM] + [VM] * 8,
        out_specs=(VM,) * 5,
        scratch_shapes=[
            pltpu.VMEM((2, quarter, D), BF),
            pltpu.VMEM((2, 2 * half // 256, 256, 256), F32),
        ],
        compiler_params=params(22),
        cost_estimate=cost(7e9, 6e6),
        name="late",
    )(meta, *slices, gain, own_w, keys, values)


def last(meta, q, keys_0, values_0, keys_1, values_1, after):
    quarter = q.shape[1]
    return pl.pallas_call(
        last_kernel,
        out_shape=jax.ShapeDtypeStruct((4, quarter // 2, 128), BF),
        in_specs=[SM] + [VM] * 5 + [AN],
        out_specs=VM,
        scratch_shapes=[pltpu.VMEM((2, 4 * quarter // 256, 256, 256), F32)],
        compiler_params=params(18),
        cost_estimate=cost(5e9, 6e6),
        name="last",
    )(meta, q, keys_0, values_0, keys_1, values_1, after)


def mlp_kernel(kept, start, meta_ref, after_ref, early_ref, res0_ref, res1_ref, *refs):
    late_refs = refs[:-7]
    wo_ref, gain_ref, wi_ref, wd_ref, out_ref, att_ref, res_ref = refs[-7:]
    count = out_ref.shape[0]
    rows = slice(start, start + count)
    second = lax.shift_right_logical(meta_ref[0], 1)

    @pl.when(second == (1 if kept else 0))
    def _():
        piece = late_refs[0].shape[1]
        for at, ref in enumerate(late_refs):
            for pair in range(4):
                att_ref[at * piece : at * piece + piece, pair * 128 : pair * 128 + 128] = ref[pair]
        res_ref[...] = res1_ref[rows, :]

    @pl.when(second == (0 if kept else 1))
    def _():
        for pair in range(4):
            att_ref[:, pair * 128 : pair * 128 + 128] = early_ref[pair, rows, :]
        res_ref[...] = res0_ref[rows, :]

    hidden = (res_ref[...].astype(F32) + dot(att_ref[...], wo_ref[...])).astype(BF)
    hidden = hidden.astype(F32)
    scale = lax.rsqrt(jnp.mean(hidden * hidden, axis=1, keepdims=True) + 1e-06)
    normed = (hidden * scale * gain_ref[...]).astype(BF)
    acc = hidden
    step = 512
    for k in range(FF // step):
        gate = dot(normed, wi_ref[:, k * step : k * step + step])
        up = dot(normed, wi_ref[:, FF + k * step : FF + k * step + step])
        half = 0.5 * gate
        act = ((half + half * jnp.tanh(half)) * up).astype(BF)
        acc = acc + dot(act, wd_ref[k * step : k * step + step, :])
    out_ref[...] = acc.astype(BF)


def mlp(kept, start, meta, after, att_0, res_0, res_1, lates, weights):
    count = sum(x.shape[1] for x in lates)
    return pl.pallas_call(
        functools.partial(mlp_kernel, kept, start),
        out_shape=jax.ShapeDtypeStruct((count, D), BF),
        in_specs=[SM, AN] + [VM] * (7 + len(lates)),
        out_specs=VM,
        scratch_shapes=[pltpu.VMEM((count, D), BF), pltpu.VMEM((count, D), BF)],
        compiler_params=params(20),
        cost_estimate=cost(count * 7e6, 6e6),
        name="mlp",
    )(meta, after, att_0, res_0, res_1, *lates, *weights)


def exchange(x, pairs):
    return lax.ppermute(x, "cols", pairs)


def local(token_ids, lengths, table, attn_gain, w_qkv, w_out, mlp_gain, w_in, w_down):
    batch_dev, quarter = token_ids.shape
    owners = lax.axis_size("rows")
    col_count = lax.axis_size("cols")
    half = 2 * quarter
    c = lax.axis_index("cols")
    h = c // 2
    row_bits = (table.shape[0] - 1).bit_length()
    meta = jnp.stack([c, jnp.where(h == 0, lengths[0], lengths[1])]).astype(I32)

    copies = jnp.broadcast_to(token_ids, (col_count, *token_ids.shape))
    ids = lax.all_to_all(copies, "cols", split_axis=0, concat_axis=0, tiled=True)
    ids = jnp.transpose(ids, (1, 0, 2)).reshape(batch_dev * col_count, quarter)
    slots, requests = route(ids, row_bits, owners)
    asked = lax.all_to_all(
        requests.reshape(owners, REQ), "rows", split_axis=0, concat_axis=0, tiled=True
    )
    looked = lookup(asked.reshape(-1), table, owners)
    got = lax.all_to_all(looked, "rows", split_axis=0, concat_axis=0, tiled=True)
    got = got.reshape(owners * CAP, table.shape[1])
    slots = slots.reshape(-1)

    theirs_0, wide = pick_first(meta, slots, got, half, quarter)
    crossed_0 = exchange(theirs_0, CROSS)
    mine_0 = pick_more(meta, slots, wide, theirs_0, half, quarter, False, 0)
    swapped_0 = exchange(mine_0, SWAP)
    theirs_1 = pick_more(meta, slots, wide, mine_0, half, quarter, True, 1)
    crossed_1 = exchange(theirs_1, CROSS)
    relayed_0 = exchange(crossed_0, SWAP)
    mine_1 = pick_more(meta, slots, wide, crossed_0, half, quarter, False, 1)
    swapped_1 = exchange(mine_1, SWAP)
    relayed_1 = exchange(crossed_1, SWAP)

    gain = attn_gain.reshape(col_count, -1)
    keys_0, values_0, own_w, att_0, res_0 = early(
        meta, (mine_0, swapped_0, crossed_0, relayed_0), gain, w_qkv, quarter
    )
    keys_1, values_1, q, att_1a, res_1 = late(
        meta, (mine_1, swapped_1, crossed_1, relayed_1), gain, own_w, keys_0, values_0, quarter
    )
    weights = (w_out, mlp_gain.reshape(1, -1), w_in, w_down)
    sent_a = mlp(False, 0, meta, res_1, att_0, res_0, res_1, (att_1a,), weights)
    came_a = exchange(sent_a, CROSS)
    att_1b = last(meta, q, keys_0, values_0, keys_1, values_1, sent_a)
    sent_b = mlp(False, quarter // 2, meta, att_1b, att_0, res_0, res_1, (att_1b,), weights)
    came_b = exchange(sent_b, CROSS)
    kept = mlp(True, 0, meta, sent_b, att_0, res_0, res_1, (att_1a, att_1b), weights)
    which = lax.broadcasted_iota(I32, (batch_dev, quarter // 2, D), 0) == h
    return jnp.concatenate(
        [
            jnp.where(which, kept[None, : quarter // 2], came_a[None]),
            jnp.where(which, kept[None, quarter // 2 :], came_b[None]),
        ],
        axis=1,
    )


def solution(mesh):
    in_specs = (P("rows", "cols"), P("rows"), P("rows", "cols"), P(), P(), P(), P(), P(), P())
    out_specs = P("rows", "cols", None)
    return jax.shard_map(local, mesh=mesh, in_specs=in_specs, out_specs=out_specs, check_vma=False)
```

```python
import functools

import jax
import jax.numpy as jnp
from jax import lax
from jax.experimental import pallas as pl
from jax.experimental.pallas import tpu as pltpu
from jax.sharding import PartitionSpec as P

D = 512
FF = 2048
CAP = 344
REQ = 384
LOG2E = 1.4426950408889634
SWAP = [(0, 1), (1, 0), (2, 3), (3, 2)]
CROSS = [(0, 3), (3, 0), (1, 2), (2, 1)]
VM = pl.BlockSpec(memory_space=pltpu.VMEM)
SM = pl.BlockSpec(memory_space=pltpu.SMEM)
AN = pl.BlockSpec(memory_space=pl.ANY)
F32 = jnp.float32
BF = jnp.bfloat16
I32 = jnp.int32


def dot(a, b):
    return lax.dot_general(a, b, (((1,), (0,)), ((), ())), preferred_element_type=F32)


def dot_t(a, b):
    return lax.dot_general(a, b, (((1,), (1,)), ((), ())), preferred_element_type=F32)


def cost(flops, moved=0):
    return pl.CostEstimate(flops=int(flops), bytes_accessed=int(moved), transcendentals=0)


def params(mib):
    return pltpu.CompilerParams(vmem_limit_bytes=mib * 1024 * 1024)


def route_kernel(row_bits, owners, ids_ref, slot_ref, req_ref):
    rows, width = ids_ref.shape
    parts = REQ // 128
    upper = (
        lax.broadcasted_iota(I32, (width, width), 0) < lax.broadcasted_iota(I32, (width, width), 1)
    ).astype(BF)
    owner_iota = lax.broadcasted_iota(I32, (owners, width), 0)
    group_iota = lax.broadcasted_iota(I32, (owners * parts, width), 0)
    lane_iota = lax.broadcasted_iota(I32, (128, width), 0)
    carry = jnp.zeros((owners, 1), F32)
    total = jnp.zeros((owners * parts, 256), F32)
    for r in range(rows):
        ids = ids_ref[r : r + 1, :]
        owner = lax.shift_right_logical(ids, row_bits)
        offset = ids & ((1 << row_bits) - 1)
        hot = (owner_iota == owner).astype(F32)
        before = dot(hot.astype(BF), upper) + carry
        rank = jnp.sum(hot * before, axis=0, keepdims=True).astype(I32)
        carry = carry + jnp.sum(hot, axis=1, keepdims=True)
        slot_ref[r : r + 1, :] = owner * CAP + rank
        place = rank + 1
        group = owner * parts + lax.shift_right_logical(place, 7)
        in_group = (group_iota == group).astype(BF)
        at_lane = lane_iota == (place & 127)
        high = jnp.where(at_lane, lax.shift_right_logical(offset, 7), 0).astype(F32).astype(BF)
        low = jnp.where(at_lane, offset & 127, 0).astype(F32).astype(BF)
        total = total + dot_t(in_group, jnp.concatenate([high, low], axis=0))
    count = carry.astype(I32)
    first_group = (
        lax.broadcasted_iota(I32, (owners * parts, owners), 0)
        == lax.broadcasted_iota(I32, (owners * parts, owners), 1) * parts
    ).astype(BF)
    lane = lax.broadcasted_iota(I32, (owners, 256), 1)
    digits = jnp.where(
        lane == 0,
        lax.shift_right_logical(count, 7),
        jnp.where(lane == 128, count & 127, 0),
    )
    total = total + dot(first_group, digits.astype(F32).astype(BF))
    req_ref[...] = total[:, :128].astype(I32) * 128 + total[:, 128:].astype(I32)


def route(ids, row_bits, owners):
    return pl.pallas_call(
        functools.partial(route_kernel, row_bits, owners),
        out_shape=(
            jax.ShapeDtypeStruct(ids.shape, I32),
            jax.ShapeDtypeStruct((owners * (REQ // 128), 128), I32),
        ),
        in_specs=[VM],
        out_specs=(VM, VM),
        compiler_params=params(16),
        name="route",
    )(ids)


def lookup_kernel(
    asked_ref, table_ref, out_ref,
    ask_ref, part_ref, wide_ref, row_ref, send_ref, ask_sem, in_sem, out_sem,
):
    owners = out_ref.shape[0]
    chunks, step, _ = part_ref.shape
    batches = 4
    batch = owners // batches

    def ask(i):
        at = pl.ds(i * batch * REQ, batch * REQ)
        return pltpu.make_async_copy(asked_ref.at[at], ask_ref.at[at], ask_sem.at[i])

    def fetch(i):
        return pltpu.make_async_copy(table_ref.at[pl.ds(i * step, step)], part_ref.at[i], in_sem.at[i])

    def store(d):
        return pltpu.make_async_copy(send_ref.at[d], out_ref.at[d], out_sem.at[d])

    for i in range(chunks):
        fetch(i).start()
    for i in range(batches):
        ask(i).start()
    piece = 512
    for i in range(chunks):
        fetch(i).wait()

        def widen(j, _):
            at = pl.multiple_of(j * piece, piece)
            wide_ref[pl.ds(i * step + at, piece), :] = part_ref[i, pl.ds(at, piece), :].astype(F32)
            return 0

        lax.fori_loop(0, step // piece, widen, 0)

    def one(d, _):
        start = d * REQ
        groups = lax.shift_right_logical(ask_ref[start] + 31, 5)

        def some(i, _):
            base = pl.multiple_of(i * 32, 32)
            first = start + base + 1
            for k in range(32):
                row_ref[pl.ds(base + k, 1), :] = wide_ref[pl.ds(ask_ref[first + k], 1), :]
            return 0

        lax.fori_loop(0, groups, some, 0)

        def narrow(i, _):
            at = pl.ds(pl.multiple_of(i * 32, 32), 32)
            send_ref[d, at, :] = row_ref[at, :].astype(BF)
            return 0

        lax.fori_loop(0, jnp.minimum(groups, CAP // 32), narrow, 0)

        @pl.when(groups > CAP // 32)
        def _():
            at = slice(CAP // 32 * 32, CAP)
            send_ref[d, at, :] = row_ref[at, :].astype(BF)

        store(d).start()
        return 0

    for i in range(batches):
        ask(i).wait()
        lax.fori_loop(i * batch, i * batch + batch, one, 0)

    def finish(d, _):
        store(d).wait()
        return 0

    lax.fori_loop(0, owners, finish, 0)


def lookup(asked, table, owners):
    rows, width = table.shape
    chunks = 8
    return pl.pallas_call(
        lookup_kernel,
        out_shape=jax.ShapeDtypeStruct((owners, CAP, width), BF),
        in_specs=[AN, AN],
        out_specs=AN,
        scratch_shapes=[
            pltpu.SMEM((owners * REQ,), I32),
            pltpu.VMEM((chunks, rows // chunks, width), BF),
            pltpu.VMEM((rows, width), F32),
            pltpu.VMEM((352, width), F32),
            pltpu.VMEM((owners, CAP, width), BF),
            pltpu.SemaphoreType.DMA((4,)),
            pltpu.SemaphoreType.DMA((chunks,)),
            pltpu.SemaphoreType.DMA((owners,)),
        ],
        compiler_params=params(62),
        cost_estimate=cost(6e9, 4e6),
        name="lookup",
    )(asked, table)


def slots_of(other, late, slot_ref, here_ref, sem):
    half = here_ref.shape[0]
    history = lax.shift_right_logical(lax.axis_index("cols"), 1)
    history = 1 - history if other else history
    start = pl.multiple_of((history * 2 + late) * half, half)
    return pltpu.make_async_copy(slot_ref.at[pl.ds(start, half)], here_ref, sem)


def pick(here_ref, start, wide_ref, row_ref, out_ref):
    block = row_ref.shape[0]
    for j in range(out_ref.shape[0] // block):

        def some(i, _):
            base = pl.multiple_of(i * 32, 32)
            at = start + j * block + base
            for k in range(32):
                row_ref[pl.ds(base + k, 1), :] = wide_ref[pl.ds(here_ref[at + k], 1), :]
            return 0

        lax.fori_loop(0, block // 32, some, 0)
        out_ref[j * block : j * block + block, :] = row_ref[...].astype(BF)


def pick_first_kernel(slot_ref, got_ref, out_ref, wide_ref, row_ref, here_ref, sem):
    step = 2 * CAP
    copy = slots_of(True, 0, slot_ref, here_ref, sem)
    copy.start()

    def widen(i, _):
        at = pl.ds(pl.multiple_of(i * step, step), step)
        wide_ref[at, :] = got_ref[at, :].astype(F32)
        return 0

    lax.fori_loop(0, wide_ref.shape[0] // step, widen, 0)
    copy.wait()
    pick(here_ref, 0, wide_ref, row_ref, out_ref)


def pick_more_kernel(which, slot_ref, wide_ref, after_ref, *refs):
    outs, (row_ref, here_ref, sem) = refs[: len(which)], refs[len(which) :]
    half = outs[0].shape[0]
    copies = [
        slots_of(other, late, slot_ref, here_ref.at[pl.ds(i * half, half)], sem.at[i])
        for i, (other, late) in enumerate(which)
    ]
    for copy in copies:
        copy.start()
    for i, copy in enumerate(copies):
        copy.wait()
        pick(here_ref, i * half, wide_ref, row_ref, outs[i])


def pick_first(slots, got, half, quarter):
    rows, width = got.shape
    return pl.pallas_call(
        pick_first_kernel,
        out_shape=(
            jax.ShapeDtypeStruct((half, width), BF),
            jax.ShapeDtypeStruct((rows, width), F32),
        ),
        in_specs=[AN, VM],
        out_specs=(VM, VM),
        scratch_shapes=[
            pltpu.VMEM((quarter, width), F32),
            pltpu.SMEM((half,), I32),
            pltpu.SemaphoreType.DMA,
        ],
        compiler_params=params(14),
        cost_estimate=cost(3e9, 4e6),
        name="pick_first",
    )(slots, got)


def pick_more(slots, wide, after, half, quarter, which):
    width = wide.shape[1]
    return pl.pallas_call(
        functools.partial(pick_more_kernel, which),
        out_shape=[jax.ShapeDtypeStruct((half, width), BF) for _ in which],
        in_specs=[AN, VM, AN],
        out_specs=[VM for _ in which],
        scratch_shapes=[
            pltpu.VMEM((quarter, width), F32),
            pltpu.SMEM((len(which) * half,), I32),
            pltpu.SemaphoreType.DMA((len(which),)),
        ],
        compiler_params=params(14),
        cost_estimate=cost(2e9 * len(which), 4e6),
        name="pick_more",
    )(slots, wide, after)


def project(c, slices, gain_ref, w_ref, norm_ref, k_ref, v_ref, res_ref, mine):
    n = norm_ref.shape[1]
    odd = c & 1
    first = lax.shift_right_logical(c, 1)
    blocks = (first, 1 - first)
    w_rows = [pl.ds(pl.multiple_of(i * 256, 256), 256) for i in blocks]

    def project_rows(normed, part):
        return dot(normed[0], w_ref[w_rows[0], part]) + dot(normed[1], w_ref[w_rows[1], part])

    for b in range(2):
        rows = slice(b * n, b * n + n)
        x0, x1, x2, x3 = [ref[rows, :].astype(F32) for ref in slices]
        square = x0 * x0 + x1 * x1 + x2 * x2 + x3 * x3
        scale = lax.rsqrt(jnp.sum(square, axis=1, keepdims=True) * (1.0 / D) + 1e-06)
        wide = (
            jnp.concatenate([jnp.where(odd == 1, x1, x0), jnp.where(odd == 1, x0, x1)], axis=1),
            jnp.concatenate([jnp.where(odd == 1, x2, x3), jnp.where(odd == 1, x3, x2)], axis=1),
        )

        @pl.when(mine == b)
        def _():
            for x, lanes in zip(wide, w_rows):
                res_ref[:, lanes] = x.astype(BF)

        normed = [
            (x * scale * gain_ref[pl.ds(i, 1), :]).astype(BF) for x, i in zip(wide, blocks)
        ]
        norm_ref[b, :, 0:256] = normed[0]
        norm_ref[b, :, 256:512] = normed[1]
        for pair in range(4):
            if pair % 2 == 0:
                keys = project_rows(normed, slice(D + pair * 128, D + pair * 128 + 256))
                values = project_rows(normed, slice(2 * D + pair * 128, 2 * D + pair * 128 + 256))
            part = slice(pair % 2 * 128, pair % 2 * 128 + 128)
            k_ref[pair, rows, :] = keys[:, part].astype(BF)
            v_ref[pair, rows, 0:128] = values[:, part].astype(BF)
            v_ref[pair, rows, 128:256] = jnp.ones((n, 128), BF)
    chosen = (norm_ref[mine, :, 0:256], norm_ref[mine, :, 256:512])
    return (project_rows(chosen, slice(0, D)) * (0.125 * LOG2E)).astype(BF)


def keep_queries(q, q_ref):
    for pair in range(4):
        q_ref[pair] = q[:, pair * 128 : pair * 128 + 128]


def attend(quarter, length, q_ref, keys, values, s_ref, out_ref, skip=0):
    size = s_ref.shape[2]
    subs = q_ref.shape[1] // size
    todo = out_ref.shape[1] // size
    per_half = keys[0].shape[1] // size
    lane = lax.broadcasted_iota(I32, (size, 128), 1)
    row = lax.broadcasted_iota(I32, (size, size), 0)
    col = lax.broadcasted_iota(I32, (size, size), 1)

    def item(it, _):
        pair = it & 3
        at_sub = lax.shift_right_logical(it, 2)
        put = pl.ds(pl.multiple_of(at_sub * size, size), size)
        rows = pl.ds(pl.multiple_of((at_sub + skip) * size, size), size)
        block = quarter * subs + at_sub + skip
        need = jnp.minimum(block + 1, lax.shift_right_logical(length + size - 1, 8))

        def body(n):
            qp = q_ref[pair, rows, :]
            limit = jnp.minimum(block * size + row + 1, length) - (n - 1) * size
            tops = []
            for head in range(2):
                qh = jnp.where((lane < 64) == (head == 0), qp, jnp.zeros_like(qp))
                m = None
                for j in range(n):
                    at = slice(j % per_half * size, j % per_half * size + size)
                    s = dot_t(qh, keys[j // per_half][pair, at, :])
                    if j == n - 1:
                        s = jnp.where(col < limit, s, -1e30)
                    s_ref[head, j] = s
                    t = jnp.maximum(s[:, 0:128], s[:, 128:256])
                    m = t if m is None else jnp.maximum(m, t)
                tops.append(jnp.max(m, axis=1, keepdims=True))
            outs = []
            for head in range(2):
                acc = None
                for j in range(n):
                    at = slice(j % per_half * size, j % per_half * size + size)
                    p = jnp.exp2(s_ref[head, j] - tops[head]).astype(BF)
                    d = dot(p, values[j // per_half][pair, at, :])
                    acc = d if acc is None else acc + d
                outs.append(acc[:, :128] / acc[:, 128:])
            out_ref[pair, put, :] = jnp.where(lane < 64, outs[0], outs[1]).astype(BF)

        for n in range(1, s_ref.shape[1] + 1):
            pl.when(need == n)(functools.partial(body, n))
        return 0

    lax.fori_loop(0, 4 * todo, item, 0)


def early_kernel(
    length_ref, s0, s1, s2, s3, gain_ref, w_ref,
    k_ref, v_ref, att_ref, res_ref, norm_ref, q_ref, s_ref,
):
    c = lax.axis_index("cols")
    quarter = jnp.minimum(c, 3 - c)
    q = project(c, (s0, s1, s2, s3), gain_ref, w_ref, norm_ref, k_ref, v_ref, res_ref, quarter)
    keep_queries(q, q_ref)
    attend(quarter, length_ref[c // 2], q_ref, (k_ref,), (v_ref,), s_ref, att_ref)


def late_kernel(
    length_ref, s0, s1, s2, s3, gain_ref, w_ref, k0_ref, v0_ref,
    k_ref, v_ref, q_ref, att_ref, res_ref, norm_ref, s_ref,
):
    c = lax.axis_index("cols")
    quarter = jnp.maximum(c, 3 - c)
    q = project(c, (s0, s1, s2, s3), gain_ref, w_ref, norm_ref, k_ref, v_ref, res_ref, quarter - 2)
    keep_queries(q, q_ref)
    attend(
        quarter, length_ref[c // 2], q_ref, (k0_ref, k_ref), (v0_ref, v_ref), s_ref, att_ref
    )


def last_kernel(length_ref, q_ref, k0_ref, v0_ref, k_ref, v_ref, after_ref, att_ref, s_ref):
    c = lax.axis_index("cols")
    quarter = jnp.maximum(c, 3 - c)
    attend(
        quarter, length_ref[c // 2], q_ref, (k0_ref, k_ref), (v0_ref, v_ref), s_ref, att_ref, 1
    )


def early(lengths, slices, gain, w_qkv, quarter):
    half = 2 * quarter
    return pl.pallas_call(
        early_kernel,
        out_shape=(
            jax.ShapeDtypeStruct((4, half, 128), BF),
            jax.ShapeDtypeStruct((4, half, 256), BF),
            jax.ShapeDtypeStruct((4, quarter, 128), BF),
            jax.ShapeDtypeStruct((quarter, D), BF),
        ),
        in_specs=[SM] + [VM] * 6,
        out_specs=(VM,) * 4,
        scratch_shapes=[
            pltpu.VMEM((2, quarter, D), BF),
            pltpu.VMEM((4, quarter, 128), BF),
            pltpu.VMEM((2, half // 256, 256, 256), F32),
        ],
        compiler_params=params(20),
        cost_estimate=cost(7e9, 6e6),
        name="early",
    )(lengths, *slices, gain, w_qkv)


def late(lengths, slices, gain, w_qkv, keys, values, quarter):
    half = 2 * quarter
    return pl.pallas_call(
        late_kernel,
        out_shape=(
            jax.ShapeDtypeStruct((4, half, 128), BF),
            jax.ShapeDtypeStruct((4, half, 256), BF),
            jax.ShapeDtypeStruct((4, quarter, 128), BF),
            jax.ShapeDtypeStruct((4, quarter // 2, 128), BF),
            jax.ShapeDtypeStruct((quarter, D), BF),
        ),
        in_specs=[SM] + [VM] * 8,
        out_specs=(VM,) * 5,
        scratch_shapes=[
            pltpu.VMEM((2, quarter, D), BF),
            pltpu.VMEM((2, 2 * half // 256, 256, 256), F32),
        ],
        compiler_params=params(22),
        cost_estimate=cost(7e9, 6e6),
        name="late",
    )(lengths, *slices, gain, w_qkv, keys, values)


def last(lengths, q, keys_0, values_0, keys_1, values_1, after):
    quarter = q.shape[1]
    return pl.pallas_call(
        last_kernel,
        out_shape=jax.ShapeDtypeStruct((4, quarter // 2, 128), BF),
        in_specs=[SM] + [VM] * 5 + [AN],
        out_specs=VM,
        scratch_shapes=[pltpu.VMEM((2, 4 * quarter // 256, 256, 256), F32)],
        compiler_params=params(18),
        cost_estimate=cost(5e9, 6e6),
        name="last",
    )(lengths, q, keys_0, values_0, keys_1, values_1, after)


def mlp_kernel(kept, start, after_ref, early_ref, res0_ref, res1_ref, *refs):
    late_refs = refs[:-7]
    wo_ref, gain_ref, wi_ref, wd_ref, out_ref, att_ref, res_ref = refs[-7:]
    count = out_ref.shape[0]
    rows = slice(start, start + count)
    second = lax.shift_right_logical(lax.axis_index("cols"), 1)

    @pl.when(second == (1 if kept else 0))
    def _():
        piece = late_refs[0].shape[1]
        for at, ref in enumerate(late_refs):
            for pair in range(4):
                att_ref[at * piece : at * piece + piece, pair * 128 : pair * 128 + 128] = ref[pair]
        res_ref[...] = res1_ref[rows, :]

    @pl.when(second == (0 if kept else 1))
    def _():
        for pair in range(4):
            att_ref[:, pair * 128 : pair * 128 + 128] = early_ref[pair, rows, :]
        res_ref[...] = res0_ref[rows, :]

    hidden = (res_ref[...].astype(F32) + dot(att_ref[...], wo_ref[...])).astype(BF)
    hidden = hidden.astype(F32)
    scale = lax.rsqrt(jnp.mean(hidden * hidden, axis=1, keepdims=True) + 1e-06)
    normed = (hidden * scale * gain_ref[...]).astype(BF)
    acc = hidden
    step = 512
    for k in range(FF // step):
        gate = dot(normed, wi_ref[:, k * step : k * step + step])
        up = dot(normed, wi_ref[:, FF + k * step : FF + k * step + step])
        half = 0.5 * gate
        act = ((half + half * jnp.tanh(half)) * up).astype(BF)
        acc = acc + dot(act, wd_ref[k * step : k * step + step, :])
    out_ref[...] = acc.astype(BF)


def mlp(kept, start, after, att_0, res_0, res_1, lates, weights):
    count = sum(x.shape[1] for x in lates)
    return pl.pallas_call(
        functools.partial(mlp_kernel, kept, start),
        out_shape=jax.ShapeDtypeStruct((count, D), BF),
        in_specs=[AN] + [VM] * (7 + len(lates)),
        out_specs=VM,
        scratch_shapes=[pltpu.VMEM((count, D), BF), pltpu.VMEM((count, D), BF)],
        compiler_params=params(20),
        cost_estimate=cost(count * 7e6, 6e6),
        name="mlp",
    )(after, att_0, res_0, res_1, *lates, *weights)


def exchange(x, pairs):
    return lax.ppermute(x, "cols", pairs)


def local(token_ids, lengths, table, attn_gain, w_qkv, w_out, mlp_gain, w_in, w_down):
    batch_dev, quarter = token_ids.shape
    owners = lax.axis_size("rows")
    col_count = lax.axis_size("cols")
    half = 2 * quarter
    c = lax.axis_index("cols")
    h = c // 2
    row_bits = (table.shape[0] - 1).bit_length()

    copies = jnp.broadcast_to(token_ids, (col_count, *token_ids.shape))
    ids = lax.all_to_all(copies, "cols", split_axis=0, concat_axis=0, tiled=True)
    ids = jnp.transpose(ids, (1, 0, 2)).reshape(batch_dev * col_count, quarter)
    slots, requests = route(ids, row_bits, owners)
    asked = lax.all_to_all(
        requests.reshape(owners, REQ), "rows", split_axis=0, concat_axis=0, tiled=True
    )
    looked = lookup(asked.reshape(-1), table, owners)
    got = lax.all_to_all(looked, "rows", split_axis=0, concat_axis=0, tiled=True)
    got = got.reshape(owners * CAP, table.shape[1])
    slots = slots.reshape(-1)

    theirs_0, wide = pick_first(slots, got, half, quarter)
    crossed_0 = exchange(theirs_0, CROSS)
    (mine_0,) = pick_more(slots, wide, theirs_0, half, quarter, ((False, 0),))
    swapped_0 = exchange(mine_0, SWAP)
    (theirs_1,) = pick_more(slots, wide, mine_0, half, quarter, ((True, 1),))
    crossed_1 = exchange(theirs_1, CROSS)
    relayed_0 = exchange(crossed_0, SWAP)
    (mine_1,) = pick_more(slots, wide, crossed_0, half, quarter, ((False, 1),))
    swapped_1 = exchange(mine_1, SWAP)
    relayed_0, crossed_1 = lax.optimization_barrier((relayed_0, crossed_1))
    relayed_1 = exchange(crossed_1, SWAP)

    gain = attn_gain.reshape(2, -1)
    keys_0, values_0, att_0, res_0 = early(
        lengths, (mine_0, swapped_0, crossed_0, relayed_0), gain, w_qkv, quarter
    )
    keys_1, values_1, q, att_1a, res_1 = late(
        lengths, (mine_1, swapped_1, crossed_1, relayed_1), gain, w_qkv, keys_0, values_0, quarter
    )
    weights = (w_out, mlp_gain.reshape(1, -1), w_in, w_down)
    sent_a = mlp(False, 0, res_1, att_0, res_0, res_1, (att_1a,), weights)
    came_a = exchange(sent_a, CROSS)
    att_1b = last(lengths, q, keys_0, values_0, keys_1, values_1, sent_a)
    sent_b = mlp(False, quarter // 2, att_1b, att_0, res_0, res_1, (att_1b,), weights)
    came_b = exchange(sent_b, CROSS)
    kept = mlp(True, 0, sent_b, att_0, res_0, res_1, (att_1a, att_1b), weights)
    which = lax.broadcasted_iota(I32, (batch_dev, quarter // 2, D), 0) == h
    return jnp.concatenate(
        [
            jnp.where(which, kept[None, : quarter // 2], came_a[None]),
            jnp.where(which, kept[None, quarter // 2 :], came_b[None]),
        ],
        axis=1,
    )


def solution(mesh):
    in_specs = (P("rows", "cols"), P("rows"), P("rows", "cols"), P(), P(), P(), P(), P(), P())
    out_specs = P("rows", "cols", None)
    return jax.shard_map(local, mesh=mesh, in_specs=in_specs, out_specs=out_specs, check_vma=False)
```

```python
import functools

import jax
import jax.numpy as jnp
from jax import lax
from jax.experimental import pallas as pl
from jax.experimental.pallas import tpu as pltpu
from jax.sharding import PartitionSpec as P

D = 512
FF = 2048
CAP = 344
REQ = 384
LOG2E = 1.4426950408889634
SWAP = [(0, 1), (1, 0), (2, 3), (3, 2)]
CROSS = [(0, 3), (3, 0), (1, 2), (2, 1)]
VM = pl.BlockSpec(memory_space=pltpu.VMEM)
SM = pl.BlockSpec(memory_space=pltpu.SMEM)
AN = pl.BlockSpec(memory_space=pl.ANY)
F32 = jnp.float32
BF = jnp.bfloat16
I32 = jnp.int32


def dot(a, b):
    return lax.dot_general(a, b, (((1,), (0,)), ((), ())), preferred_element_type=F32)


def dot_t(a, b):
    return lax.dot_general(a, b, (((1,), (1,)), ((), ())), preferred_element_type=F32)


def cost(flops, moved=0):
    return pl.CostEstimate(flops=int(flops), bytes_accessed=int(moved), transcendentals=0)


def params(mib):
    return pltpu.CompilerParams(vmem_limit_bytes=mib * 1024 * 1024)


def route_kernel(row_bits, owners, ids_ref, slot_ref, req_ref):
    rows, width = ids_ref.shape
    parts = REQ // 128
    upper = (
        lax.broadcasted_iota(I32, (width, width), 0) < lax.broadcasted_iota(I32, (width, width), 1)
    ).astype(BF)
    owner_iota = lax.broadcasted_iota(I32, (owners, width), 0)
    group_iota = lax.broadcasted_iota(I32, (owners * parts, width), 0)
    lane_iota = lax.broadcasted_iota(I32, (128, width), 0)
    carry = jnp.zeros((owners, 1), F32)
    total = jnp.zeros((owners * parts, 256), F32)
    for r in range(rows):
        ids = ids_ref[r : r + 1, :]
        owner = lax.shift_right_logical(ids, row_bits)
        offset = ids & ((1 << row_bits) - 1)
        hot = (owner_iota == owner).astype(F32)
        before = dot(hot.astype(BF), upper) + carry
        rank = jnp.sum(hot * before, axis=0, keepdims=True).astype(I32)
        carry = carry + jnp.sum(hot, axis=1, keepdims=True)
        slot_ref[r : r + 1, :] = owner * CAP + rank
        place = rank + 1
        group = owner * parts + lax.shift_right_logical(place, 7)
        in_group = (group_iota == group).astype(BF)
        at_lane = lane_iota == (place & 127)
        high = jnp.where(at_lane, lax.shift_right_logical(offset, 7), 0).astype(F32).astype(BF)
        low = jnp.where(at_lane, offset & 127, 0).astype(F32).astype(BF)
        total = total + dot_t(in_group, jnp.concatenate([high, low], axis=0))
    count = carry.astype(I32)
    first_group = (
        lax.broadcasted_iota(I32, (owners * parts, owners), 0)
        == lax.broadcasted_iota(I32, (owners * parts, owners), 1) * parts
    ).astype(BF)
    lane = lax.broadcasted_iota(I32, (owners, 256), 1)
    digits = jnp.where(
        lane == 0,
        lax.shift_right_logical(count, 7),
        jnp.where(lane == 128, count & 127, 0),
    )
    total = total + dot(first_group, digits.astype(F32).astype(BF))
    req_ref[...] = total[:, :128].astype(I32) * 128 + total[:, 128:].astype(I32)


def route(ids, row_bits, owners):
    return pl.pallas_call(
        functools.partial(route_kernel, row_bits, owners),
        out_shape=(
            jax.ShapeDtypeStruct(ids.shape, I32),
            jax.ShapeDtypeStruct((owners * (REQ // 128), 128), I32),
        ),
        in_specs=[VM],
        out_specs=(VM, VM),
        compiler_params=params(16),
        name="route",
    )(ids)


def lookup_kernel(
    asked_ref, table_ref, out_ref,
    ask_ref, part_ref, wide_ref, row_ref, send_ref, ask_sem, in_sem, out_sem,
):
    owners = out_ref.shape[0]
    chunks, step, _ = part_ref.shape
    batches = 4
    batch = owners // batches

    def ask(i):
        at = pl.ds(i * batch * REQ, batch * REQ)
        return pltpu.make_async_copy(asked_ref.at[at], ask_ref.at[at], ask_sem.at[i])

    def fetch(i):
        return pltpu.make_async_copy(table_ref.at[pl.ds(i * step, step)], part_ref.at[i], in_sem.at[i])

    def store(d):
        return pltpu.make_async_copy(send_ref.at[d], out_ref.at[d], out_sem.at[d])

    for i in range(chunks):
        fetch(i).start()
    for i in range(batches):
        ask(i).start()
    piece = 512
    for i in range(chunks):
        fetch(i).wait()

        def widen(j, _):
            at = pl.multiple_of(j * piece, piece)
            wide_ref[pl.ds(i * step + at, piece), :] = part_ref[i, pl.ds(at, piece), :].astype(F32)
            return 0

        lax.fori_loop(0, step // piece, widen, 0)

    def one(d, _):
        start = d * REQ
        groups = lax.shift_right_logical(ask_ref[start] + 31, 5)

        def narrow(i):
            at = pl.ds(pl.multiple_of(i * 32, 32), 32)
            send_ref[d, at, :] = row_ref[at, :].astype(BF)

        def some(i, _):
            base = pl.multiple_of(i * 32, 32)
            first = start + base + 1
            narrow(jnp.maximum(i - 1, 0))
            for k in range(32):
                row_ref[pl.ds(base + k, 1), :] = wide_ref[pl.ds(ask_ref[first + k], 1), :]
            return 0

        lax.fori_loop(0, groups, some, 0)
        narrow(jnp.clip(groups - 1, 0, CAP // 32 - 1))

        @pl.when(groups > CAP // 32)
        def _():
            at = slice(CAP // 32 * 32, CAP)
            send_ref[d, at, :] = row_ref[at, :].astype(BF)

        store(d).start()
        return 0

    for i in range(batches):
        ask(i).wait()
        lax.fori_loop(i * batch, i * batch + batch, one, 0)

    def finish(d, _):
        store(d).wait()
        return 0

    lax.fori_loop(0, owners, finish, 0)


def lookup(asked, table, owners):
    rows, width = table.shape
    chunks = 8
    return pl.pallas_call(
        lookup_kernel,
        out_shape=jax.ShapeDtypeStruct((owners, CAP, width), BF),
        in_specs=[AN, AN],
        out_specs=AN,
        scratch_shapes=[
            pltpu.SMEM((owners * REQ,), I32),
            pltpu.VMEM((chunks, rows // chunks, width), BF),
            pltpu.VMEM((rows, width), F32),
            pltpu.VMEM((352, width), F32),
            pltpu.VMEM((owners, CAP, width), BF),
            pltpu.SemaphoreType.DMA((4,)),
            pltpu.SemaphoreType.DMA((chunks,)),
            pltpu.SemaphoreType.DMA((owners,)),
        ],
        compiler_params=params(62),
        cost_estimate=cost(6e9, 4e6),
        name="lookup",
    )(asked, table)


def slots_of(other, late, slot_ref, here_ref, sem):
    half = here_ref.shape[0]
    history = lax.shift_right_logical(lax.axis_index("cols"), 1)
    history = 1 - history if other else history
    start = pl.multiple_of((history * 2 + late) * half, half)
    return pltpu.make_async_copy(slot_ref.at[pl.ds(start, half)], here_ref, sem)


def pick(here_ref, start, wide_ref, row_ref, out_ref):
    block = row_ref.shape[0]
    for j in range(out_ref.shape[0] // block):

        def some(i, _):
            base = pl.multiple_of(i * 32, 32)
            at = start + j * block + base
            for k in range(32):
                row_ref[pl.ds(base + k, 1), :] = wide_ref[pl.ds(here_ref[at + k], 1), :]
            return 0

        lax.fori_loop(0, block // 32, some, 0)
        out_ref[j * block : j * block + block, :] = row_ref[...].astype(BF)


def pick_first_kernel(slot_ref, got_ref, out_ref, wide_ref, row_ref, here_ref, sem):
    step = 2 * CAP
    copy = slots_of(True, 0, slot_ref, here_ref, sem)
    copy.start()

    def widen(i, _):
        at = pl.ds(pl.multiple_of(i * step, step), step)
        wide_ref[at, :] = got_ref[at, :].astype(F32)
        return 0

    lax.fori_loop(0, wide_ref.shape[0] // step, widen, 0)
    copy.wait()
    pick(here_ref, 0, wide_ref, row_ref, out_ref)


def pick_more_kernel(which, slot_ref, wide_ref, after_ref, *refs):
    outs, (row_ref, here_ref, sem) = refs[: len(which)], refs[len(which) :]
    half = outs[0].shape[0]
    copies = [
        slots_of(other, late, slot_ref, here_ref.at[pl.ds(i * half, half)], sem.at[i])
        for i, (other, late) in enumerate(which)
    ]
    for copy in copies:
        copy.start()
    for i, copy in enumerate(copies):
        copy.wait()
        pick(here_ref, i * half, wide_ref, row_ref, outs[i])


def pick_first(slots, got, half, quarter):
    rows, width = got.shape
    return pl.pallas_call(
        pick_first_kernel,
        out_shape=(
            jax.ShapeDtypeStruct((half, width), BF),
            jax.ShapeDtypeStruct((rows, width), F32),
        ),
        in_specs=[AN, VM],
        out_specs=(VM, VM),
        scratch_shapes=[
            pltpu.VMEM((quarter, width), F32),
            pltpu.SMEM((half,), I32),
            pltpu.SemaphoreType.DMA,
        ],
        compiler_params=params(14),
        cost_estimate=cost(3e9, 4e6),
        name="pick_first",
    )(slots, got)


def pick_more(slots, wide, after, half, quarter, which):
    width = wide.shape[1]
    return pl.pallas_call(
        functools.partial(pick_more_kernel, which),
        out_shape=[jax.ShapeDtypeStruct((half, width), BF) for _ in which],
        in_specs=[AN, VM, AN],
        out_specs=[VM for _ in which],
        scratch_shapes=[
            pltpu.VMEM((quarter, width), F32),
            pltpu.SMEM((len(which) * half,), I32),
            pltpu.SemaphoreType.DMA((len(which),)),
        ],
        compiler_params=params(14),
        cost_estimate=cost(2e9 * len(which), 4e6),
        name="pick_more",
    )(slots, wide, after)


def project(c, slices, gain_ref, w_ref, wv_ref, norm_ref, k_ref, v_ref, res_ref, mine):
    n = norm_ref.shape[1]
    odd = c & 1
    first = lax.shift_right_logical(c, 1)
    blocks = (first, 1 - first)
    w_rows = [pl.ds(pl.multiple_of(i * 256, 256), 256) for i in blocks]

    def project_rows(normed, part):
        return dot(normed[0], w_ref[w_rows[0], part]) + dot(normed[1], w_ref[w_rows[1], part])

    for b in range(2):
        rows = slice(b * n, b * n + n)
        x0, x1, x2, x3 = [ref[rows, :].astype(F32) for ref in slices]
        square = x0 * x0 + x1 * x1 + x2 * x2 + x3 * x3
        scale = lax.rsqrt(jnp.sum(square, axis=1, keepdims=True) * (1.0 / D) + 1e-06)
        wide = (
            jnp.concatenate([jnp.where(odd == 1, x1, x0), jnp.where(odd == 1, x0, x1)], axis=1),
            jnp.concatenate([jnp.where(odd == 1, x2, x3), jnp.where(odd == 1, x3, x2)], axis=1),
        )

        @pl.when(mine == b)
        def _():
            for x, lanes in zip(wide, w_rows):
                res_ref[:, lanes] = x.astype(BF)

        normed = [
            (x * scale * gain_ref[pl.ds(i, 1), :]).astype(BF) for x, i in zip(wide, blocks)
        ]
        norm_ref[b, :, 0:256] = normed[0]
        norm_ref[b, :, 256:512] = normed[1]
        for pair in range(0, 4, 2):
            keys = project_rows(normed, slice(D + pair * 128, D + pair * 128 + 256))
            k_ref[pair, rows, :] = keys[:, 0:128].astype(BF)
            k_ref[pair + 1, rows, :] = keys[:, 128:256].astype(BF)
            cols = slice(pair * 128, pair * 128 + 256)
            values = dot_t(wv_ref[cols, w_rows[0]], normed[0]) + dot_t(
                wv_ref[cols, w_rows[1]], normed[1]
            )
            for i in range(4):
                v_ref[2 * pair + i, 0:64, rows] = values[64 * i : 64 * i + 64, :].astype(BF)
                v_ref[2 * pair + i, 64:80, rows] = jnp.ones((16, n), BF)
    chosen = (norm_ref[mine, :, 0:256], norm_ref[mine, :, 256:512])
    return (project_rows(chosen, slice(0, D)) * (0.125 * LOG2E)).astype(BF)


def keep_queries(q, q_ref):
    for pair in range(4):
        q_ref[pair] = q[:, pair * 128 : pair * 128 + 128]


def attend(quarter, length, q_ref, keys, values, s_ref, out_ref, skip=0):
    size = s_ref.shape[2]
    subs = q_ref.shape[1] // size
    todo = out_ref.shape[1] // size
    per_half = keys[0].shape[1] // size
    lane = lax.broadcasted_iota(I32, (size, 128), 1)
    row = lax.broadcasted_iota(I32, (size, size), 0)
    col = lax.broadcasted_iota(I32, (size, size), 1)

    def item(it, _):
        pair = it & 3
        at_sub = lax.shift_right_logical(it, 2)
        put = pl.ds(pl.multiple_of(at_sub * size, size), size)
        rows = pl.ds(pl.multiple_of((at_sub + skip) * size, size), size)
        block = quarter * subs + at_sub + skip
        need = jnp.minimum(block + 1, lax.shift_right_logical(length + size - 1, 8))

        def body(n):
            qp = q_ref[pair, rows, :]
            limit = jnp.minimum(block * size + col + 1, length) - (n - 1) * size
            tops = []
            for head in range(2):
                qh = jnp.where((lane < 64) == (head == 0), qp, jnp.zeros_like(qp))
                m = None
                for j in range(n):
                    at = slice(j % per_half * size, j % per_half * size + size)
                    s = dot_t(keys[j // per_half][pair, at, :], qh)
                    if j == n - 1:
                        s = jnp.where(row < limit, s, -1e30)
                    s_ref[head, j] = s
                    t = jnp.max(s.reshape(size // 8, 8, size), axis=0)
                    m = t if m is None else jnp.maximum(m, t)
                tops.append(jnp.max(m, axis=0, keepdims=True))
            outs = []
            for head in range(2):
                acc = None
                for j in range(n):
                    at = slice(j % per_half * size, j % per_half * size + size)
                    p = jnp.exp2(s_ref[head, j] - tops[head]).astype(BF)
                    d = dot(values[j // per_half][2 * pair + head, :, at], p)
                    acc = d if acc is None else acc + d
                outs.append(acc[0:64, :] / acc[64:65, :])
            out_ref[pair, put, :] = jnp.transpose(jnp.concatenate(outs, axis=0)).astype(BF)

        for n in range(1, s_ref.shape[1] + 1):
            pl.when(need == n)(functools.partial(body, n))
        return 0

    lax.fori_loop(0, 4 * todo, item, 0)


def early_kernel(
    length_ref, s0, s1, s2, s3, gain_ref, w_ref, wv_ref,
    k_ref, v_ref, att_ref, res_ref, norm_ref, q_ref, s_ref,
):
    c = lax.axis_index("cols")
    quarter = jnp.minimum(c, 3 - c)
    q = project(c, (s0, s1, s2, s3), gain_ref, w_ref, wv_ref, norm_ref, k_ref, v_ref, res_ref, quarter)
    keep_queries(q, q_ref)
    attend(quarter, length_ref[c // 2], q_ref, (k_ref,), (v_ref,), s_ref, att_ref)


def late_kernel(
    length_ref, s0, s1, s2, s3, gain_ref, w_ref, wv_ref, k0_ref, v0_ref,
    k_ref, v_ref, q_ref, att_ref, res_ref, norm_ref, s_ref,
):
    c = lax.axis_index("cols")
    quarter = jnp.maximum(c, 3 - c)
    q = project(
        c, (s0, s1, s2, s3), gain_ref, w_ref, wv_ref, norm_ref, k_ref, v_ref, res_ref, quarter - 2
    )
    keep_queries(q, q_ref)
    attend(
        quarter, length_ref[c // 2], q_ref, (k0_ref, k_ref), (v0_ref, v_ref), s_ref, att_ref
    )


def last_kernel(length_ref, q_ref, k0_ref, v0_ref, k_ref, v_ref, after_ref, att_ref, s_ref):
    c = lax.axis_index("cols")
    quarter = jnp.maximum(c, 3 - c)
    attend(
        quarter, length_ref[c // 2], q_ref, (k0_ref, k_ref), (v0_ref, v_ref), s_ref, att_ref, 1
    )


def early(lengths, slices, gain, w_qkv, w_values, quarter):
    half = 2 * quarter
    return pl.pallas_call(
        early_kernel,
        out_shape=(
            jax.ShapeDtypeStruct((4, half, 128), BF),
            jax.ShapeDtypeStruct((8, 80, half), BF),
            jax.ShapeDtypeStruct((4, quarter, 128), BF),
            jax.ShapeDtypeStruct((quarter, D), BF),
        ),
        in_specs=[SM] + [VM] * 7,
        out_specs=(VM,) * 4,
        scratch_shapes=[
            pltpu.VMEM((2, quarter, D), BF),
            pltpu.VMEM((4, quarter, 128), BF),
            pltpu.VMEM((2, half // 256, 256, 256), F32),
        ],
        compiler_params=params(20),
        cost_estimate=cost(7e9, 6e6),
        name="early",
    )(lengths, *slices, gain, w_qkv, w_values)


def late(lengths, slices, gain, w_qkv, w_values, keys, values, quarter):
    half = 2 * quarter
    return pl.pallas_call(
        late_kernel,
        out_shape=(
            jax.ShapeDtypeStruct((4, half, 128), BF),
            jax.ShapeDtypeStruct((8, 80, half), BF),
            jax.ShapeDtypeStruct((4, quarter, 128), BF),
            jax.ShapeDtypeStruct((4, quarter // 2, 128), BF),
            jax.ShapeDtypeStruct((quarter, D), BF),
        ),
        in_specs=[SM] + [VM] * 9,
        out_specs=(VM,) * 5,
        scratch_shapes=[
            pltpu.VMEM((2, quarter, D), BF),
            pltpu.VMEM((2, 2 * half // 256, 256, 256), F32),
        ],
        compiler_params=params(22),
        cost_estimate=cost(7e9, 6e6),
        name="late",
    )(lengths, *slices, gain, w_qkv, w_values, keys, values)


def last(lengths, q, keys_0, values_0, keys_1, values_1, after):
    quarter = q.shape[1]
    return pl.pallas_call(
        last_kernel,
        out_shape=jax.ShapeDtypeStruct((4, quarter // 2, 128), BF),
        in_specs=[SM] + [VM] * 5 + [AN],
        out_specs=VM,
        scratch_shapes=[pltpu.VMEM((2, 4 * quarter // 256, 256, 256), F32)],
        compiler_params=params(18),
        cost_estimate=cost(5e9, 6e6),
        name="last",
    )(lengths, q, keys_0, values_0, keys_1, values_1, after)


def mlp_kernel(kept, start, after_ref, early_ref, res0_ref, res1_ref, *refs):
    late_refs = refs[:-7]
    wo_ref, gain_ref, wi_ref, wd_ref, out_ref, att_ref, res_ref = refs[-7:]
    count = out_ref.shape[0]
    rows = slice(start, start + count)
    second = lax.shift_right_logical(lax.axis_index("cols"), 1)

    @pl.when(second == (1 if kept else 0))
    def _():
        piece = late_refs[0].shape[1]
        for at, ref in enumerate(late_refs):
            for pair in range(4):
                att_ref[at * piece : at * piece + piece, pair * 128 : pair * 128 + 128] = ref[pair]
        res_ref[...] = res1_ref[rows, :]

    @pl.when(second == (0 if kept else 1))
    def _():
        for pair in range(4):
            att_ref[:, pair * 128 : pair * 128 + 128] = early_ref[pair, rows, :]
        res_ref[...] = res0_ref[rows, :]

    hidden = (res_ref[...].astype(F32) + dot(att_ref[...], wo_ref[...])).astype(BF)
    hidden = hidden.astype(F32)
    scale = lax.rsqrt(jnp.mean(hidden * hidden, axis=1, keepdims=True) + 1e-06)
    normed = (hidden * scale * gain_ref[...]).astype(BF)
    acc = hidden
    step = 512
    for k in range(FF // step):
        gate = dot(normed, wi_ref[:, k * step : k * step + step])
        up = dot(normed, wi_ref[:, FF + k * step : FF + k * step + step])
        half = 0.5 * gate
        act = ((half + half * jnp.tanh(half)) * up).astype(BF)
        acc = acc + dot(act, wd_ref[k * step : k * step + step, :])
    out_ref[...] = acc.astype(BF)


def mlp(kept, start, after, att_0, res_0, res_1, lates, weights):
    count = sum(x.shape[1] for x in lates)
    return pl.pallas_call(
        functools.partial(mlp_kernel, kept, start),
        out_shape=jax.ShapeDtypeStruct((count, D), BF),
        in_specs=[AN] + [VM] * (7 + len(lates)),
        out_specs=VM,
        scratch_shapes=[pltpu.VMEM((count, D), BF), pltpu.VMEM((count, D), BF)],
        compiler_params=params(20),
        cost_estimate=cost(count * 7e6, 6e6),
        name="mlp",
    )(after, att_0, res_0, res_1, *lates, *weights)


def exchange(x, pairs):
    return lax.ppermute(x, "cols", pairs)


def local(token_ids, lengths, table, attn_gain, w_qkv, w_out, mlp_gain, w_in, w_down):
    batch_dev, quarter = token_ids.shape
    owners = lax.axis_size("rows")
    col_count = lax.axis_size("cols")
    half = 2 * quarter
    c = lax.axis_index("cols")
    h = c // 2
    row_bits = (table.shape[0] - 1).bit_length()

    copies = jnp.broadcast_to(token_ids, (col_count, *token_ids.shape))
    ids = lax.all_to_all(copies, "cols", split_axis=0, concat_axis=0, tiled=True)
    ids = jnp.transpose(ids, (1, 0, 2)).reshape(batch_dev * col_count, quarter)
    slots, requests = route(ids, row_bits, owners)
    asked = lax.all_to_all(
        requests.reshape(owners, REQ), "rows", split_axis=0, concat_axis=0, tiled=True
    )
    looked = lookup(asked.reshape(-1), table, owners)
    got = lax.all_to_all(looked, "rows", split_axis=0, concat_axis=0, tiled=True)
    got = got.reshape(owners * CAP, table.shape[1])
    slots = slots.reshape(-1)

    theirs_0, wide = pick_first(slots, got, half, quarter)
    crossed_0 = exchange(theirs_0, CROSS)
    (mine_0,) = pick_more(slots, wide, theirs_0, half, quarter, ((False, 0),))
    swapped_0 = exchange(mine_0, SWAP)
    (theirs_1,) = pick_more(slots, wide, mine_0, half, quarter, ((True, 1),))
    crossed_1 = exchange(theirs_1, CROSS)
    relayed_0 = exchange(crossed_0, SWAP)
    (mine_1,) = pick_more(slots, wide, crossed_0, half, quarter, ((False, 1),))
    swapped_1 = exchange(mine_1, SWAP)
    relayed_0, crossed_1 = lax.optimization_barrier((relayed_0, crossed_1))
    relayed_1 = exchange(crossed_1, SWAP)

    gain = attn_gain.reshape(2, -1)
    w_values = jnp.transpose(w_qkv[:, 2 * D :])
    keys_0, values_0, att_0, res_0 = early(
        lengths, (mine_0, swapped_0, crossed_0, relayed_0), gain, w_qkv, w_values, quarter
    )
    keys_1, values_1, q, att_1a, res_1 = late(
        lengths, (mine_1, swapped_1, crossed_1, relayed_1), gain, w_qkv, w_values, keys_0, values_0, quarter
    )
    weights = (w_out, mlp_gain.reshape(1, -1), w_in, w_down)
    sent_a = mlp(False, 0, res_1, att_0, res_0, res_1, (att_1a,), weights)
    came_a = exchange(sent_a, CROSS)
    att_1b = last(lengths, q, keys_0, values_0, keys_1, values_1, sent_a)
    sent_b = mlp(False, quarter // 2, att_1b, att_0, res_0, res_1, (att_1b,), weights)
    came_b = exchange(sent_b, CROSS)
    kept = mlp(True, 0, sent_b, att_0, res_0, res_1, (att_1a, att_1b), weights)
    which = lax.broadcasted_iota(I32, (batch_dev, quarter // 2, D), 0) == h
    return jnp.concatenate(
        [
            jnp.where(which, kept[None, : quarter // 2], came_a[None]),
            jnp.where(which, kept[None, quarter // 2 :], came_b[None]),
        ],
        axis=1,
    )


def solution(mesh):
    in_specs = (P("rows", "cols"), P("rows"), P("rows", "cols"), P(), P(), P(), P(), P(), P())
    out_specs = P("rows", "cols", None)
    return jax.shard_map(local, mesh=mesh, in_specs=in_specs, out_specs=out_specs, check_vma=False)
```

```python
import functools

import jax
import jax.numpy as jnp
from jax import lax
from jax.experimental import pallas as pl
from jax.experimental.pallas import tpu as pltpu
from jax.sharding import PartitionSpec as P

D = 512
FF = 2048
CAP = 344
REQ = 384
LOG2E = 1.4426950408889634
SWAP = [(0, 1), (1, 0), (2, 3), (3, 2)]
CROSS = [(0, 3), (3, 0), (1, 2), (2, 1)]
VM = pl.BlockSpec(memory_space=pltpu.VMEM)
SM = pl.BlockSpec(memory_space=pltpu.SMEM)
AN = pl.BlockSpec(memory_space=pl.ANY)
F32 = jnp.float32
BF = jnp.bfloat16
I32 = jnp.int32


def dot(a, b):
    return lax.dot_general(a, b, (((1,), (0,)), ((), ())), preferred_element_type=F32)


def dot_t(a, b):
    return lax.dot_general(a, b, (((1,), (1,)), ((), ())), preferred_element_type=F32)


def cost(flops, moved=0):
    return pl.CostEstimate(flops=int(flops), bytes_accessed=int(moved), transcendentals=0)


def params(mib):
    return pltpu.CompilerParams(vmem_limit_bytes=mib * 1024 * 1024)


def route_kernel(row_bits, owners, ids_ref, slot_ref, req_ref):
    rows, width = ids_ref.shape
    parts = REQ // 128
    upper = (
        lax.broadcasted_iota(I32, (width, width), 0) < lax.broadcasted_iota(I32, (width, width), 1)
    ).astype(BF)
    owner_iota = lax.broadcasted_iota(I32, (owners, width), 0)
    group_iota = lax.broadcasted_iota(I32, (owners * parts, width), 0)
    lane_iota = lax.broadcasted_iota(I32, (128, width), 0)
    carry = jnp.zeros((owners, 1), F32)
    total = jnp.zeros((2 * owners * parts, 128), F32)
    for r in range(rows):
        ids = ids_ref[r : r + 1, :]
        owner = lax.shift_right_logical(ids, row_bits)
        offset = ids & ((1 << row_bits) - 1)
        hot = (owner_iota == owner).astype(F32)
        before = dot(hot.astype(BF), upper) + carry
        rank = jnp.sum(hot * before, axis=0, keepdims=True).astype(I32)
        carry = carry + jnp.sum(hot, axis=1, keepdims=True)
        slot_ref[r : r + 1, :] = owner * CAP + rank
        place = rank + 1
        group = owner * parts + lax.shift_right_logical(place, 7)
        in_group = group_iota == group
        at_lane = (lane_iota == (place & 127)).astype(F32).astype(BF)
        high = jnp.where(in_group, lax.shift_right_logical(offset, 7).astype(F32), 0.0).astype(BF)
        low = jnp.where(in_group, (offset & 127).astype(F32), 0.0).astype(BF)
        total = total + dot_t(jnp.concatenate([high, low], axis=0), at_lane)
    count = carry.astype(I32)
    first_group = (
        lax.broadcasted_iota(I32, (owners * parts, owners), 0)
        == lax.broadcasted_iota(I32, (owners * parts, owners), 1) * parts
    ).astype(BF)
    lane = lax.broadcasted_iota(I32, (owners, 128), 1)
    digits = [
        jnp.where(lane == 0, digit, 0).astype(F32).astype(BF)
        for digit in (lax.shift_right_logical(count, 7), count & 127)
    ]
    half = owners * parts
    high = total[:half, :] + dot(first_group, digits[0])
    low = total[half:, :] + dot(first_group, digits[1])
    req_ref[...] = high.astype(I32) * 128 + low.astype(I32)


def route(ids, row_bits, owners):
    return pl.pallas_call(
        functools.partial(route_kernel, row_bits, owners),
        out_shape=(
            jax.ShapeDtypeStruct(ids.shape, I32),
            jax.ShapeDtypeStruct((owners * (REQ // 128), 128), I32),
        ),
        in_specs=[VM],
        out_specs=(VM, VM),
        compiler_params=params(16),
        name="route",
    )(ids)


def lookup_kernel(
    asked_ref, table_ref, out_ref,
    ask_ref, part_ref, wide_ref, row_ref, send_ref, ask_sem, in_sem, out_sem,
):
    owners = out_ref.shape[0]
    chunks, step, _ = part_ref.shape
    batches = 4
    batch = owners // batches

    def ask(i):
        at = pl.ds(i * batch * REQ, batch * REQ)
        return pltpu.make_async_copy(asked_ref.at[at], ask_ref.at[at], ask_sem.at[i])

    def fetch(i):
        return pltpu.make_async_copy(table_ref.at[pl.ds(i * step, step)], part_ref.at[i], in_sem.at[i])

    def store(d):
        return pltpu.make_async_copy(send_ref.at[d], out_ref.at[d], out_sem.at[d])

    for i in range(chunks):
        fetch(i).start()
    for i in range(batches):
        ask(i).start()
    piece = 512
    for i in range(chunks):
        fetch(i).wait()

        def widen(j, _):
            at = pl.multiple_of(j * piece, piece)
            wide_ref[pl.ds(i * step + at, piece), :] = part_ref[i, pl.ds(at, piece), :].astype(F32)
            return 0

        lax.fori_loop(0, step // piece, widen, 0)

    def one(d, _):
        start = d * REQ
        groups = lax.shift_right_logical(ask_ref[start] + 31, 5)

        def narrow(i):
            at = pl.ds(pl.multiple_of(i * 32, 32), 32)
            send_ref[d, at, :] = row_ref[at, :].astype(BF)

        def some(i, _):
            base = pl.multiple_of(i * 32, 32)
            first = start + base + 1
            narrow(jnp.maximum(i - 1, 0))
            for k in range(32):
                row_ref[pl.ds(base + k, 1), :] = wide_ref[pl.ds(ask_ref[first + k], 1), :]
            return 0

        lax.fori_loop(0, groups, some, 0)
        narrow(jnp.clip(groups - 1, 0, CAP // 32 - 1))

        @pl.when(groups > CAP // 32)
        def _():
            at = slice(CAP // 32 * 32, CAP)
            send_ref[d, at, :] = row_ref[at, :].astype(BF)

        store(d).start()
        return 0

    for i in range(batches):
        ask(i).wait()
        lax.fori_loop(i * batch, i * batch + batch, one, 0)

    def finish(d, _):
        store(d).wait()
        return 0

    lax.fori_loop(0, owners, finish, 0)


def lookup(asked, table, owners):
    rows, width = table.shape
    chunks = 16
    return pl.pallas_call(
        lookup_kernel,
        out_shape=jax.ShapeDtypeStruct((owners, CAP, width), BF),
        in_specs=[AN, AN],
        out_specs=AN,
        scratch_shapes=[
            pltpu.SMEM((owners * REQ,), I32),
            pltpu.VMEM((chunks, rows // chunks, width), BF),
            pltpu.VMEM((rows, width), F32),
            pltpu.VMEM((352, width), F32),
            pltpu.VMEM((owners, CAP, width), BF),
            pltpu.SemaphoreType.DMA((4,)),
            pltpu.SemaphoreType.DMA((chunks,)),
            pltpu.SemaphoreType.DMA((owners,)),
        ],
        compiler_params=params(62),
        cost_estimate=cost(6e9, 4e6),
        name="lookup",
    )(asked, table)


def slots_of(other, late, slot_ref, here_ref, sem):
    half = here_ref.shape[0]
    history = lax.shift_right_logical(lax.axis_index("cols"), 1)
    history = 1 - history if other else history
    start = pl.multiple_of((history * 2 + late) * half, half)
    return pltpu.make_async_copy(slot_ref.at[pl.ds(start, half)], here_ref, sem)


def pick(here_ref, start, wide_ref, row_ref, out_ref):
    block = row_ref.shape[0]
    for j in range(out_ref.shape[0] // block):

        def some(i, _):
            base = pl.multiple_of(i * 32, 32)
            at = start + j * block + base
            for k in range(32):
                row_ref[pl.ds(base + k, 1), :] = wide_ref[pl.ds(here_ref[at + k], 1), :]
            return 0

        lax.fori_loop(0, block // 32, some, 0)
        out_ref[j * block : j * block + block, :] = row_ref[...].astype(BF)


def pick_first_kernel(slot_ref, got_ref, out_ref, wide_ref, row_ref, here_ref, sem):
    step = 2 * CAP
    copy = slots_of(True, 0, slot_ref, here_ref, sem)
    copy.start()

    def widen(i, _):
        at = pl.ds(pl.multiple_of(i * step, step), step)
        wide_ref[at, :] = got_ref[at, :].astype(F32)
        return 0

    lax.fori_loop(0, wide_ref.shape[0] // step, widen, 0)
    copy.wait()
    pick(here_ref, 0, wide_ref, row_ref, out_ref)


def pick_more_kernel(which, slot_ref, wide_ref, after_ref, *refs):
    outs, (row_ref, here_ref, sem) = refs[: len(which)], refs[len(which) :]
    half = outs[0].shape[0]
    copies = [
        slots_of(other, late, slot_ref, here_ref.at[pl.ds(i * half, half)], sem.at[i])
        for i, (other, late) in enumerate(which)
    ]
    for copy in copies:
        copy.start()
    for i, copy in enumerate(copies):
        copy.wait()
        pick(here_ref, i * half, wide_ref, row_ref, outs[i])


def pick_first(slots, got, half, quarter):
    rows, width = got.shape
    return pl.pallas_call(
        pick_first_kernel,
        out_shape=(
            jax.ShapeDtypeStruct((half, width), BF),
            jax.ShapeDtypeStruct((rows, width), F32),
        ),
        in_specs=[AN, VM],
        out_specs=(VM, VM),
        scratch_shapes=[
            pltpu.VMEM((quarter, width), F32),
            pltpu.SMEM((half,), I32),
            pltpu.SemaphoreType.DMA,
        ],
        compiler_params=params(14),
        cost_estimate=cost(3e9, 4e6),
        name="pick_first",
    )(slots, got)


def pick_more(slots, wide, after, half, quarter, which):
    width = wide.shape[1]
    return pl.pallas_call(
        functools.partial(pick_more_kernel, which),
        out_shape=[jax.ShapeDtypeStruct((half, width), BF) for _ in which],
        in_specs=[AN, VM, AN],
        out_specs=[VM for _ in which],
        scratch_shapes=[
            pltpu.VMEM((quarter, width), F32),
            pltpu.SMEM((len(which) * half,), I32),
            pltpu.SemaphoreType.DMA((len(which),)),
        ],
        compiler_params=params(14),
        cost_estimate=cost(2e9 * len(which), 4e6),
        name="pick_more",
    )(slots, wide, after)


def project(c, slices, gain_ref, w_ref, wv_ref, norm_ref, k_ref, v_ref, res_ref, mine):
    n = norm_ref.shape[1]
    odd = c & 1
    first = lax.shift_right_logical(c, 1)
    blocks = (first, 1 - first)
    w_rows = [pl.ds(pl.multiple_of(i * 256, 256), 256) for i in blocks]

    def project_rows(normed, part):
        return dot(normed[0], w_ref[w_rows[0], part]) + dot(normed[1], w_ref[w_rows[1], part])

    for b in range(2):
        rows = slice(b * n, b * n + n)
        x0, x1, x2, x3 = [ref[rows, :].astype(F32) for ref in slices]
        square = x0 * x0 + x1 * x1 + x2 * x2 + x3 * x3
        scale = lax.rsqrt(jnp.sum(square, axis=1, keepdims=True) * (1.0 / D) + 1e-06)
        wide = (
            jnp.concatenate([jnp.where(odd == 1, x1, x0), jnp.where(odd == 1, x0, x1)], axis=1),
            jnp.concatenate([jnp.where(odd == 1, x2, x3), jnp.where(odd == 1, x3, x2)], axis=1),
        )

        @pl.when(mine == b)
        def _():
            for x, lanes in zip(wide, w_rows):
                res_ref[:, lanes] = x.astype(BF)

        normed = [
            (x * scale * gain_ref[pl.ds(i, 1), :]).astype(BF) for x, i in zip(wide, blocks)
        ]
        norm_ref[b, :, 0:256] = normed[0]
        norm_ref[b, :, 256:512] = normed[1]
        for pair in range(0, 4, 2):
            keys = project_rows(normed, slice(D + pair * 128, D + pair * 128 + 256))
            k_ref[pair, rows, :] = keys[:, 0:128].astype(BF)
            k_ref[pair + 1, rows, :] = keys[:, 128:256].astype(BF)
            cols = slice(pair * 128, pair * 128 + 256)
            values = dot_t(wv_ref[cols, w_rows[0]], normed[0]) + dot_t(
                wv_ref[cols, w_rows[1]], normed[1]
            )
            for i in range(4):
                v_ref[2 * pair + i, 0:64, rows] = values[64 * i : 64 * i + 64, :].astype(BF)
                v_ref[2 * pair + i, 64:80, rows] = jnp.ones((16, n), BF)
    chosen = (norm_ref[mine, :, 0:256], norm_ref[mine, :, 256:512])
    return (project_rows(chosen, slice(0, D)) * (0.125 * LOG2E)).astype(BF)


def keep_queries(q, q_ref):
    for pair in range(4):
        q_ref[pair] = q[:, pair * 128 : pair * 128 + 128]


def attend(quarter, length, q_ref, keys, values, s_ref, out_ref, skip=0):
    size = s_ref.shape[2]
    subs = q_ref.shape[1] // size
    todo = out_ref.shape[1] // size
    per_half = keys[0].shape[1] // size
    lane = lax.broadcasted_iota(I32, (size, 128), 1)
    row = lax.broadcasted_iota(I32, (size, size), 0)
    col = lax.broadcasted_iota(I32, (size, size), 1)

    def item(it, _):
        pair = it & 3
        at_sub = lax.shift_right_logical(it, 2)
        put = pl.ds(pl.multiple_of(at_sub * size, size), size)
        rows = pl.ds(pl.multiple_of((at_sub + skip) * size, size), size)
        block = quarter * subs + at_sub + skip
        need = jnp.minimum(block + 1, lax.shift_right_logical(length + size - 1, 8))

        def body(n):
            qp = q_ref[pair, rows, :]
            limit = jnp.minimum(block * size + col + 1, length) - (n - 1) * size
            tops = []
            for head in range(2):
                qh = jnp.where((lane < 64) == (head == 0), qp, jnp.zeros_like(qp))
                m = None
                for j in range(n):
                    at = slice(j % per_half * size, j % per_half * size + size)
                    s = dot_t(keys[j // per_half][pair, at, :], qh)
                    if j == n - 1:
                        s = jnp.where(row < limit, s, -1e30)
                    s_ref[head, j] = s
                    t = jnp.max(s.reshape(size // 8, 8, size), axis=0)
                    m = t if m is None else jnp.maximum(m, t)
                tops.append(jnp.max(m, axis=0, keepdims=True))
            outs = []
            for head in range(2):
                acc = None
                for j in range(n):
                    at = slice(j % per_half * size, j % per_half * size + size)
                    p = jnp.exp2(s_ref[head, j] - tops[head]).astype(BF)
                    d = dot(values[j // per_half][2 * pair + head, :, at], p)
                    acc = d if acc is None else acc + d
                outs.append(acc[0:64, :] / acc[64:65, :])
            out_ref[pair, put, :] = jnp.transpose(jnp.concatenate(outs, axis=0)).astype(BF)

        for n in range(1, s_ref.shape[1] + 1):
            pl.when(need == n)(functools.partial(body, n))
        return 0

    lax.fori_loop(0, 4 * todo, item, 0)


def early_kernel(
    length_ref, s0, s1, s2, s3, gain_ref, w_ref, wv_ref,
    k_ref, v_ref, att_ref, res_ref, norm_ref, q_ref, s_ref,
):
    c = lax.axis_index("cols")
    quarter = jnp.minimum(c, 3 - c)
    q = project(c, (s0, s1, s2, s3), gain_ref, w_ref, wv_ref, norm_ref, k_ref, v_ref, res_ref, quarter)
    keep_queries(q, q_ref)
    attend(quarter, length_ref[c // 2], q_ref, (k_ref,), (v_ref,), s_ref, att_ref)


def late_kernel(
    length_ref, s0, s1, s2, s3, gain_ref, w_ref, wv_ref, k0_ref, v0_ref,
    k_ref, v_ref, q_ref, att_ref, res_ref, norm_ref, s_ref,
):
    c = lax.axis_index("cols")
    quarter = jnp.maximum(c, 3 - c)
    q = project(
        c, (s0, s1, s2, s3), gain_ref, w_ref, wv_ref, norm_ref, k_ref, v_ref, res_ref, quarter - 2
    )
    keep_queries(q, q_ref)
    attend(
        quarter, length_ref[c // 2], q_ref, (k0_ref, k_ref), (v0_ref, v_ref), s_ref, att_ref
    )


def last_kernel(length_ref, q_ref, k0_ref, v0_ref, k_ref, v_ref, after_ref, att_ref, s_ref):
    c = lax.axis_index("cols")
    quarter = jnp.maximum(c, 3 - c)
    attend(
        quarter, length_ref[c // 2], q_ref, (k0_ref, k_ref), (v0_ref, v_ref), s_ref, att_ref, 1
    )


def early(lengths, slices, gain, w_qkv, w_values, quarter):
    half = 2 * quarter
    return pl.pallas_call(
        early_kernel,
        out_shape=(
            jax.ShapeDtypeStruct((4, half, 128), BF),
            jax.ShapeDtypeStruct((8, 80, half), BF),
            jax.ShapeDtypeStruct((4, quarter, 128), BF),
            jax.ShapeDtypeStruct((quarter, D), BF),
        ),
        in_specs=[SM] + [VM] * 7,
        out_specs=(VM,) * 4,
        scratch_shapes=[
            pltpu.VMEM((2, quarter, D), BF),
            pltpu.VMEM((4, quarter, 128), BF),
            pltpu.VMEM((2, half // 256, 256, 256), F32),
        ],
        compiler_params=params(20),
        cost_estimate=cost(7e9, 6e6),
        name="early",
    )(lengths, *slices, gain, w_qkv, w_values)


def late(lengths, slices, gain, w_qkv, w_values, keys, values, quarter):
    half = 2 * quarter
    return pl.pallas_call(
        late_kernel,
        out_shape=(
            jax.ShapeDtypeStruct((4, half, 128), BF),
            jax.ShapeDtypeStruct((8, 80, half), BF),
            jax.ShapeDtypeStruct((4, quarter, 128), BF),
            jax.ShapeDtypeStruct((4, quarter // 2, 128), BF),
            jax.ShapeDtypeStruct((quarter, D), BF),
        ),
        in_specs=[SM] + [VM] * 9,
        out_specs=(VM,) * 5,
        scratch_shapes=[
            pltpu.VMEM((2, quarter, D), BF),
            pltpu.VMEM((2, 2 * half // 256, 256, 256), F32),
        ],
        compiler_params=params(22),
        cost_estimate=cost(7e9, 6e6),
        name="late",
    )(lengths, *slices, gain, w_qkv, w_values, keys, values)


def last(lengths, q, keys_0, values_0, keys_1, values_1, after):
    quarter = q.shape[1]
    return pl.pallas_call(
        last_kernel,
        out_shape=jax.ShapeDtypeStruct((4, quarter // 2, 128), BF),
        in_specs=[SM] + [VM] * 5 + [AN],
        out_specs=VM,
        scratch_shapes=[pltpu.VMEM((2, 4 * quarter // 256, 256, 256), F32)],
        compiler_params=params(18),
        cost_estimate=cost(5e9, 6e6),
        name="last",
    )(lengths, q, keys_0, values_0, keys_1, values_1, after)


def mlp_kernel(kept, start, after_ref, early_ref, res0_ref, res1_ref, *refs):
    late_refs = refs[:-7]
    wo_ref, gain_ref, wi_ref, wd_ref, out_ref, att_ref, res_ref = refs[-7:]
    count = out_ref.shape[0]
    rows = slice(start, start + count)
    second = lax.shift_right_logical(lax.axis_index("cols"), 1)

    @pl.when(second == (1 if kept else 0))
    def _():
        piece = late_refs[0].shape[1]
        for at, ref in enumerate(late_refs):
            for pair in range(4):
                att_ref[at * piece : at * piece + piece, pair * 128 : pair * 128 + 128] = ref[pair]
        res_ref[...] = res1_ref[rows, :]

    @pl.when(second == (0 if kept else 1))
    def _():
        for pair in range(4):
            att_ref[:, pair * 128 : pair * 128 + 128] = early_ref[pair, rows, :]
        res_ref[...] = res0_ref[rows, :]

    hidden = (res_ref[...].astype(F32) + dot(att_ref[...], wo_ref[...])).astype(BF)
    hidden = hidden.astype(F32)
    scale = lax.rsqrt(jnp.mean(hidden * hidden, axis=1, keepdims=True) + 1e-06)
    normed = (hidden * scale * gain_ref[...]).astype(BF)
    acc = hidden
    step = 512
    for k in range(FF // step):
        gate = dot(normed, wi_ref[:, k * step : k * step + step])
        up = dot(normed, wi_ref[:, FF + k * step : FF + k * step + step])
        half = 0.5 * gate
        act = ((half + half * jnp.tanh(half)) * up).astype(BF)
        acc = acc + dot(act, wd_ref[k * step : k * step + step, :])
    out_ref[...] = acc.astype(BF)


def mlp(kept, start, after, att_0, res_0, res_1, lates, weights):
    count = sum(x.shape[1] for x in lates)
    return pl.pallas_call(
        functools.partial(mlp_kernel, kept, start),
        out_shape=jax.ShapeDtypeStruct((count, D), BF),
        in_specs=[AN] + [VM] * (7 + len(lates)),
        out_specs=VM,
        scratch_shapes=[pltpu.VMEM((count, D), BF), pltpu.VMEM((count, D), BF)],
        compiler_params=params(20),
        cost_estimate=cost(count * 7e6, 6e6),
        name="mlp",
    )(after, att_0, res_0, res_1, *lates, *weights)


def exchange(x, pairs):
    return lax.ppermute(x, "cols", pairs)


def local(token_ids, lengths, table, attn_gain, w_qkv, w_out, mlp_gain, w_in, w_down):
    batch_dev, quarter = token_ids.shape
    owners = lax.axis_size("rows")
    col_count = lax.axis_size("cols")
    half = 2 * quarter
    c = lax.axis_index("cols")
    h = c // 2
    row_bits = (table.shape[0] - 1).bit_length()

    copies = jnp.broadcast_to(token_ids, (col_count, *token_ids.shape))
    ids = lax.all_to_all(copies, "cols", split_axis=0, concat_axis=0, tiled=True)
    ids = jnp.transpose(ids, (1, 0, 2)).reshape(batch_dev * col_count, quarter)
    slots, requests = route(ids, row_bits, owners)
    asked = lax.all_to_all(
        requests.reshape(owners, REQ), "rows", split_axis=0, concat_axis=0, tiled=True
    )
    looked = lookup(asked.reshape(-1), table, owners)
    got = lax.all_to_all(looked, "rows", split_axis=0, concat_axis=0, tiled=True)
    got = got.reshape(owners * CAP, table.shape[1])
    slots = slots.reshape(-1)

    theirs_0, wide = pick_first(slots, got, half, quarter)
    crossed_0 = exchange(theirs_0, CROSS)
    (mine_0,) = pick_more(slots, wide, theirs_0, half, quarter, ((False, 0),))
    swapped_0 = exchange(mine_0, SWAP)
    (theirs_1,) = pick_more(slots, wide, mine_0, half, quarter, ((True, 1),))
    crossed_1 = exchange(theirs_1, CROSS)
    relayed_0 = exchange(crossed_0, SWAP)
    (mine_1,) = pick_more(slots, wide, crossed_0, half, quarter, ((False, 1),))
    swapped_1 = exchange(mine_1, SWAP)
    relayed_0, crossed_1 = lax.optimization_barrier((relayed_0, crossed_1))
    relayed_1 = exchange(crossed_1, SWAP)

    gain = attn_gain.reshape(2, -1)
    w_values = jnp.transpose(w_qkv[:, 2 * D :])
    keys_0, values_0, att_0, res_0 = early(
        lengths, (mine_0, swapped_0, crossed_0, relayed_0), gain, w_qkv, w_values, quarter
    )
    keys_1, values_1, q, att_1a, res_1 = late(
        lengths, (mine_1, swapped_1, crossed_1, relayed_1), gain, w_qkv, w_values, keys_0, values_0, quarter
    )
    weights = (w_out, mlp_gain.reshape(1, -1), w_in, w_down)
    sent_a = mlp(False, 0, res_1, att_0, res_0, res_1, (att_1a,), weights)
    came_a = exchange(sent_a, CROSS)
    att_1b = last(lengths, q, keys_0, values_0, keys_1, values_1, sent_a)
    sent_b = mlp(False, quarter // 2, att_1b, att_0, res_0, res_1, (att_1b,), weights)
    came_b = exchange(sent_b, CROSS)
    kept = mlp(True, 0, sent_b, att_0, res_0, res_1, (att_1a, att_1b), weights)
    came = jnp.concatenate([came_a, came_b], axis=0)
    which = lax.broadcasted_iota(I32, (batch_dev, quarter, D), 0) == h
    return jnp.where(which, kept[None], came[None])


def solution(mesh):
    in_specs = (P("rows", "cols"), P("rows"), P("rows", "cols"), P(), P(), P(), P(), P(), P())
    out_specs = P("rows", "cols", None)
    return jax.shard_map(local, mesh=mesh, in_specs=in_specs, out_specs=out_specs, check_vma=False)
```
